256 devices in a mesh: expert: 64 (over z, x, core), shard: 4 (over y).
Axes of the slice: x: 4, y: 4, z: 8, core: 2. Of those that a mesh axis runs over, the one named last changes fastest.
Arguments:
- master_down: float32 [128, 768, 2048], P('expert', None, 'shard'), may hold values from -0.3125 to 0.3125
- router_weight: float32 [2048, 128], P('shard', 'expert'), may hold values from -0.125 to 0.125
- router_gain: float32 [2048], P('shard'), may hold values from 0.25 to 1.75
Outputs:
- final_down: bfloat16 [128, 768, 2048], P('expert')
- scale_down: float32 [128, 768], P('expert')
- serve_router: bfloat16 [2048, 128], replicated
The draws below stay inside these ranges and needn't reach their ends.
All inputs are finite; a program needn't handle non-finite values.
Results may differ from the reference program's by a relative error of at most 0.001.
Values may be sent and summed in bfloat16 or wider, within the bound.
A program may use at most 64 MiB of HBM per device.

```python
import jax
import jax.numpy as jnp
from jax import lax

EXPERTS = 128
D_MODEL = 2048
D_EXPERT = 768


def strengthened(result, rng, source, target, blocks, factor):
    owner, partner = [(jnp.arange(result.shape[axis_at]) // (result.shape[axis_at] // blocks)).reshape([-1 if axis == axis_at else 1 for axis in range(result.ndim)]) for axis_at in (source, target)]
    chosen = jax.random.permutation(rng, blocks)[partner]
    strong = (owner == chosen) | (owner == (partner + blocks // 2) % blocks)
    return jnp.where(strong, factor * result, result)


def levels(key, extent, pieces, least, top_value):
    def one(dim, parts):
        steps = jax.random.uniform(jax.random.fold_in(jax.random.fold_in(key, 6), dim), (parts,), jnp.float32, least / len(pieces), top_value / len(pieces))
        return jnp.repeat(jnp.exp(steps), extent[dim] // parts).reshape((-1,) + (1,) * (len(extent) - dim - 1))

    factor_of = one(*pieces[0])
    for cut in pieces[1:]:
        factor_of = factor_of * one(*cut)
    return factor_of


def centred(rng, extent, spread, reach, cuts=(), held_as=jnp.bfloat16):
    drawn = jax.random.normal(rng, extent, jnp.float32) * spread
    if len(cuts) > 0:
        drawn = levels(rng, extent, cuts, -0.22, 0.18) * drawn
    return jnp.clip(drawn, min=-reach, max=reach).astype(held_as)


def bell_draw_with(rng, dims, deviation, most, pieces, heavy, held_as=jnp.bfloat16):
    drawn = deviation * jax.random.normal(rng, dims, jnp.float32)
    if pieces:
        drawn = drawn * levels(rng, dims, pieces, -0.22, 0.18)
    return jnp.clip(strengthened(drawn, jax.random.fold_in(rng, 3), *heavy), -most, most).astype(held_as)


def setup_inputs(seed: int = 0) -> dict:
    key_of = jax.random.split(jax.random.key(seed), 4)
    master_down = bell_draw_with(key_of[0], (EXPERTS, D_EXPERT, D_MODEL), D_EXPERT ** -0.5, 0.3125, ((0, 64), (2, 4)), (2, 1, 4, 2.0), jnp.float32)
    router_weight = centred(key_of[1], (D_MODEL, EXPERTS), D_MODEL ** -0.5, 0.125, ((0, 4), (1, 64)), jnp.float32)
    router_gain = jnp.clip(1.0 + 0.15 * jax.random.normal(key_of[2], (D_MODEL,), jnp.float32), 0.25, 1.75)
    return dict(master_down=master_down, router_weight=router_weight, router_gain=router_gain)


def reference(master_down, router_weight, router_gain):
    scale_down = jnp.sqrt(lax.optimization_barrier(jnp.sum(master_down * master_down, axis=2)))
    final_down = (master_down / jnp.expand_dims(scale_down, 2)).astype(jnp.bfloat16)
    serve_router = (router_weight * router_gain[:, None]).astype(jnp.bfloat16)
    return (final_down, scale_down, serve_router)
```

```python
import functools

import jax
import jax.numpy as jnp
from jax import lax
from jax.experimental import pallas as pl
from jax.experimental.pallas import tpu as pltpu
from jax.sharding import Mesh
from jax.sharding import PartitionSpec as P

MESH = pl.DeviceIdType.MESH
EXPERT = ("z", "x", "core")
BF16, F32 = jnp.bfloat16, jnp.float32

BLOCK = 128
GROUPS = BLOCK // 8
PARTS = ((0, 2), (2, 7), (7, 12))
CHUNKS = ((0, 1), (1, 2), (2, 4), (4, 6), (6, 8), (8, 10), (10, 12))
HALF = 4


def part_of(block):
    for p, (lo, hi) in enumerate(PARTS):
        if lo <= block < hi:
            return p, (block - lo) * GROUPS


def pick(first):
    lane = lax.broadcasted_iota(jnp.int32, (GROUPS, 8, 128), 2)
    group = lax.broadcasted_iota(jnp.int32, (GROUPS, 8, 128), 0)
    return lane == group + first


def column(packed, block):
    p, first = part_of(block)
    spread = jnp.where(pick(first), packed[p][None], 0.0)
    return jnp.sum(spread, axis=2, keepdims=True).reshape(BLOCK, 1)


def gather_kernel(
    master, router, gain,
    gathered, scale_out, router_out,
    rows, sums, wide, weight, gains, pieces, tall,
    load_sem, small_sem, sum_send, sum_recv, up_send, up_recv, down_send, down_recv,
    fwd_up_send, fwd_up_recv, fwd_down_send, fwd_down_recv,
    ry_send, ry_recv, rc_send, rc_recv, rx_send, rx_recv, zu_send, zu_recv, zd_send, zd_recv,
):
    z, x, core, y = (lax.axis_index(a) for a in ("z", "x", "core", "shard"))
    nz, nx, ny = 8, 4, 4
    mine = z * (nx * 2) + x * 2 + core

    def at_y(step):
        return (z, x, core, lax.rem(y + step, ny))

    def at_x(step):
        return (z, lax.rem(x + step, nx), core, y)

    def at_z(step):
        return (lax.rem(z + step, nz), x, core, y)

    partner = (z, x, 1 - core, y)

    loads = []
    for p, (lo, hi) in enumerate(PARTS):
        view = pl.ds(lo * BLOCK, (hi - lo) * BLOCK)
        loads.append(pltpu.make_async_copy(master.at[view], rows.at[view], load_sem.at[p]))
        loads[-1].start()
    small = [
        pltpu.make_async_copy(router, weight, small_sem.at[0]),
        pltpu.make_async_copy(gain, gains, small_sem.at[1]),
    ]
    for copy in small:
        copy.start()

    barrier = pltpu.get_barrier_semaphore()
    peers = [at_y(1), at_y(2), at_y(3), at_x(1), at_x(2), at_x(3), partner, at_z(1), at_z(nz - 1)]
    for peer in peers:
        pl.semaphore_signal(barrier, inc=1, device_id=peer, device_id_type=MESH)

    def remote(src, dst, send, recv, peer):
        copy = pltpu.make_async_remote_copy(
            src_ref=src, dst_ref=dst, send_sem=send, recv_sem=recv, device_id=peer, device_id_type=MESH
        )
        return copy

    def partial_sums(p):
        lo, hi = PARTS[p]
        loads[p].wait()
        packed = jnp.zeros((8, 128), F32)
        for block in range(lo, hi):
            values = rows[pl.ds(block * BLOCK, BLOCK), :]
            total = jnp.sum(values * values, axis=1, keepdims=True).reshape(GROUPS, 8, 1)
            packed = packed + jnp.sum(jnp.where(pick((block - lo) * GROUPS), total, 0.0), axis=0)
        sums[y, p] = packed

    def send_sums(first, count, slot):
        out = []
        for d in (1, 3, 2):
            view = sums.at[y, pl.ds(first, count)]
            out.append(remote(view, view, sum_send.at[slot, d - 1], sum_recv.at[slot, d - 1], at_y(d)))
            out[-1].start()
        return out

    partial_sums(0)
    for copy in small:
        copy.wait()
    pieces[y, mine] = (weight[...] * gains[...]).astype(BF16)
    pl.semaphore_wait(barrier, len(peers))
    sum_copies = [send_sums(0, 1, 0)]
    partial_sums(1)
    partial_sums(2)
    sum_copies.append(send_sums(1, 2, 1))

    view = pieces.at[y, mine]
    ry = [remote(view, view, ry_send.at[d - 1], ry_recv.at[d - 1], at_y(d)) for d in (1, 2, 3)]
    for copy in ry:
        copy.start()

    inverse = {}

    def finish_sums(slot, parts):
        for copy in sum_copies[slot]:
            copy.wait_recv()
        for p in parts:
            scale = jnp.sqrt((sums[0, p] + sums[1, p]) + (sums[2, p] + sums[3, p]))
            wide[p] = scale
            inverse[p] = 1.0 / scale

    def chunk_view(owner, c):
        lo, hi = CHUNKS[c]
        return gathered.at[owner, pl.ds(lo * BLOCK, (hi - lo) * BLOCK)]

    bulk = []
    finish_sums(0, (0,))
    for c, (lo, hi) in enumerate(CHUNKS):
        if lo == PARTS[1][0]:
            finish_sums(1, (1, 2))
        for block in range(lo, hi):
            view = pl.ds(block * BLOCK, BLOCK)
            gathered[y, view, :] = (rows[view, :] * column(inverse, block)).astype(BF16)
        view = chunk_view(y, c)
        bulk.append(remote(view, view, up_send.at[c], up_recv.at[c], at_y(1)))
        bulk.append(remote(view, view, down_send.at[c], down_recv.at[c], at_y(3)))
        bulk[-2].start()
        bulk[-1].start()

    for copy in ry:
        copy.wait_recv()
    view = pieces.at[:, mine]
    rc = remote(view, view, rc_send, rc_recv, partner)
    rc.start()
    scales = [wide[p] for p in range(len(PARTS))]
    for block in range(12):
        same = lax.broadcasted_iota(jnp.int32, (BLOCK, 128), 0) == lax.broadcasted_iota(jnp.int32, (BLOCK, 128), 1)
        line = jnp.sum(jnp.where(same, column(scales, block), 0.0), axis=0, keepdims=True)
        scale_out[block // 6 : block // 6 + 1, (block % 6) * 128 : (block % 6 + 1) * 128] = line
    rc.wait_recv()
    view = pieces.at[:, pl.ds(z * 8 + x * 2, 2)]
    rx = [remote(view, view, rx_send.at[d - 1], rx_recv.at[d - 1], at_x(d)) for d in (1, 2, 3)]
    for copy in rx:
        copy.start()
    for copy in rx:
        copy.wait_recv()
    zu, zd = [], []
    for k in range(4):
        if k:
            zu[-1].wait_recv()
        view = pieces.at[:, pl.ds(lax.rem(z + nz - k, nz) * 8, 8)]
        zu.append(remote(view, view, zu_send.at[k], zu_recv.at[k], at_z(1)))
        zu[-1].start()
        if k < 3:
            if k:
                zd[-1].wait_recv()
            view = pieces.at[:, pl.ds(lax.rem(z + k, nz) * 8, 8)]
            zd.append(remote(view, view, zd_send.at[k], zd_recv.at[k], at_z(nz - 1)))
            zd[-1].start()

    forwards = []
    for k in range(HALF):
        bulk[2 * k].wait_recv()
        view = chunk_view(lax.rem(y + 3, ny), k)
        forwards.append(remote(view, view, fwd_up_send.at[k], fwd_up_recv.at[k], at_y(1)))
        forwards[-1].start()
        if k + HALF < len(CHUNKS):
            c = k + HALF
            bulk[2 * c + 1].wait_recv()
            view = chunk_view(lax.rem(y + 1, ny), c)
            forwards.append(remote(view, view, fwd_down_send.at[k], fwd_down_recv.at[k], at_y(3)))
            forwards[-1].start()

    zu[-1].wait_recv()
    zd[-1].wait_recv()

    def lay(step, _):
        for s in range(ny):
            four = [pieces[s, step * 4 + i].astype(F32) for i in range(4)]
            tall[pl.ds(pl.multiple_of(step * 8, 8), 8), s * 512 : (s + 1) * 512] = jnp.concatenate(four, axis=0)
        return 0

    lax.fori_loop(0, 16, lay, 0)
    for i in range(16):
        router_out[i * 128 : (i + 1) * 128, :] = tall[:, i * 128 : (i + 1) * 128].T.astype(BF16)

    for c in range(len(CHUNKS)):
        if c >= HALF:
            bulk[2 * c].wait_recv()
        else:
            bulk[2 * c + 1].wait_recv()
    for copy in forwards:
        copy.wait_recv()
    for copy in bulk + forwards + ry + [rc] + rx + zu + zd:
        copy.wait_send()
    for copies in sum_copies:
        for copy in copies:
            copy.wait_send()


def write_kernel(gathered, scale, router, down_out, scale_out, router_out, sems):
    copies = [
        pltpu.make_async_copy(gathered.at[s], down_out.at[:, pl.ds(s * 512, 512)], sems.at[s]) for s in range(4)
    ]
    copies.append(pltpu.make_async_copy(scale, scale_out, sems.at[4]))
    copies.append(pltpu.make_async_copy(router, router_out, sems.at[5]))
    for copy in copies:
        copy.start()
    for copy in copies:
        copy.wait()


def body(master_down, router_weight, router_gain):
    dma = pltpu.SemaphoreType.DMA
    n = len(CHUNKS)
    hbm = pl.BlockSpec(memory_space=pltpu.HBM)
    vmem = pl.BlockSpec(memory_space=pltpu.VMEM)
    gathered, scale, router = pl.pallas_call(
        gather_kernel,
        name="gather",
        out_shape=(
            pltpu.VMEM((4, 1536, 512), BF16),
            pltpu.VMEM((2, 768), F32),
            pltpu.VMEM((2048, 128), BF16),
        ),
        in_specs=[hbm] * 3,
        out_specs=[vmem] * 3,
        scratch_shapes=[
            pltpu.VMEM((1536, 512), F32),
            pltpu.VMEM((4, 3, 8, 128), F32),
            pltpu.VMEM((3, 8, 128), F32),
            pltpu.VMEM((2, 512), F32),
            pltpu.VMEM((1, 512), F32),
            pltpu.VMEM((4, 64, 2, 512), BF16),
            pltpu.VMEM((128, 2048), F32),
            dma((3,)), dma((2,)), dma((2, 3)), dma((2, 3)), dma((n,)), dma((n,)), dma((n,)), dma((n,)),
            dma((HALF,)), dma((HALF,)), dma((HALF,)), dma((HALF,)),
            dma((3,)), dma((3,)), dma(()), dma(()), dma((3,)), dma((3,)), dma((4,)), dma((4,)), dma((3,)), dma((3,)),
        ],
        compiler_params=pltpu.CompilerParams(collective_id=0, has_side_effects=True, vmem_limit_bytes=32 << 20),
    )(master_down.reshape(1536, 512), router_weight.T, router_gain.reshape(1, 512))
    down, scale, router = pl.pallas_call(
        write_kernel,
        name="write",
        out_shape=(
            jax.ShapeDtypeStruct((1536, 2048), BF16),
            jax.ShapeDtypeStruct((2, 768), F32),
            jax.ShapeDtypeStruct((2048, 128), BF16),
        ),
        in_specs=[vmem] * 3,
        out_specs=[hbm] * 3,
        scratch_shapes=[dma((6,))],
    )(gathered, scale, router)
    return down.reshape(2, 768, 2048), scale, router


def solution(mesh):
    finer = Mesh(mesh.devices.reshape(8, 4, 2, mesh.shape["shard"]), (*EXPERT, "shard"))
    in_specs = (P(EXPERT, None, "shard"), P("shard", EXPERT), P("shard"))
    out_specs = (P(EXPERT, None, None), P(EXPERT, None), P())
    return jax.shard_map(body, mesh=finer, in_specs=in_specs, out_specs=out_specs, check_vma=False)
```

```python
import functools

import jax
import jax.numpy as jnp
from jax import lax
from jax.experimental import pallas as pl
from jax.experimental.pallas import tpu as pltpu
from jax.sharding import Mesh
from jax.sharding import PartitionSpec as P

MESH = pl.DeviceIdType.MESH
EXPERT = ("z", "x", "core")
BF16, F32 = jnp.bfloat16, jnp.float32

BLOCK = 128
GROUPS = BLOCK // 8
PARTS = ((0, 2), (2, 7), (7, 12))
CHUNKS = ((0, 1), (1, 2), (2, 4), (4, 6), (6, 8), (8, 10), (10, 12))
HALF = 4


def part_of(block):
    for p, (lo, hi) in enumerate(PARTS):
        if lo <= block < hi:
            return p, (block - lo) * GROUPS


def pick(first):
    lane = lax.broadcasted_iota(jnp.int32, (GROUPS, 8, 128), 2)
    group = lax.broadcasted_iota(jnp.int32, (GROUPS, 8, 128), 0)
    return lane == group + first


def column(packed, block):
    p, first = part_of(block)
    spread = jnp.where(pick(first), packed[p][None], 0.0)
    return jnp.sum(spread, axis=2, keepdims=True).reshape(BLOCK, 1)


def gather_kernel(
    master, router, gain,
    gathered, scale_out, router_out,
    rows, sums, wide, weight, gains, pieces, tall,
    load_sem, small_sem, sum_send, sum_recv, up_send, up_recv, down_send, down_recv,
    fwd_up_send, fwd_up_recv, fwd_down_send, fwd_down_recv,
    ry_send, ry_recv, rc_send, rc_recv, rx_send, rx_recv, zu_send, zu_recv, zd_send, zd_recv,
):
    z, x, core, y = (lax.axis_index(a) for a in ("z", "x", "core", "shard"))
    nz, nx, ny = 8, 4, 4
    mine = z * (nx * 2) + x * 2 + core

    def at_y(step):
        return (z, x, core, lax.rem(y + step, ny))

    def at_x(step):
        return (z, lax.rem(x + step, nx), core, y)

    def at_z(step):
        return (lax.rem(z + step, nz), x, core, y)

    partner = (z, x, 1 - core, y)

    loads = []
    for p, (lo, hi) in enumerate(PARTS):
        view = pl.ds(lo * BLOCK, (hi - lo) * BLOCK)
        loads.append(pltpu.make_async_copy(master.at[view], rows.at[view], load_sem.at[p]))
        loads[-1].start()
    small = [
        pltpu.make_async_copy(router, weight, small_sem.at[0]),
        pltpu.make_async_copy(gain, gains, small_sem.at[1]),
    ]
    for copy in small:
        copy.start()

    barrier = pltpu.get_barrier_semaphore()
    peers = [at_y(1), at_y(2), at_y(3), at_x(1), at_x(2), at_x(3), partner, at_z(1), at_z(nz - 1)]
    for peer in peers:
        pl.semaphore_signal(barrier, inc=1, device_id=peer, device_id_type=MESH)

    def remote(src, dst, send, recv, peer):
        copy = pltpu.make_async_remote_copy(
            src_ref=src, dst_ref=dst, send_sem=send, recv_sem=recv, device_id=peer, device_id_type=MESH
        )
        return copy

    def partial_sums(p):
        lo, hi = PARTS[p]
        loads[p].wait()
        packed = jnp.zeros((8, 128), F32)
        for block in range(lo, hi):
            values = rows[pl.ds(block * BLOCK, BLOCK), :]
            total = jnp.sum(values * values, axis=1, keepdims=True).reshape(GROUPS, 8, 1)
            packed = packed + jnp.sum(jnp.where(pick((block - lo) * GROUPS), total, 0.0), axis=0)
        sums[y, p] = packed

    def send_sums(first, count, slot):
        out = []
        for d in (1, 3, 2):
            view = sums.at[y, pl.ds(first, count)]
            out.append(remote(view, view, sum_send.at[slot, d - 1], sum_recv.at[slot, d - 1], at_y(d)))
            out[-1].start()
        return out

    partial_sums(0)
    for copy in small:
        copy.wait()
    pieces[y, mine] = (weight[...] * gains[...]).astype(BF16)
    pl.semaphore_wait(barrier, len(peers))
    sum_copies = [send_sums(0, 1, 0)]
    partial_sums(1)
    partial_sums(2)
    sum_copies.append(send_sums(1, 2, 1))

    view = pieces.at[y, mine]
    ry = [remote(view, view, ry_send.at[d - 1], ry_recv.at[d - 1], at_y(d)) for d in (1, 2, 3)]
    for copy in ry:
        copy.start()

    inverse = {}

    def finish_sums(slot, parts):
        for copy in sum_copies[slot]:
            copy.wait_recv()
        for p in parts:
            scale = jnp.sqrt((sums[0, p] + sums[1, p]) + (sums[2, p] + sums[3, p]))
            wide[p] = scale
            inverse[p] = 1.0 / scale

    def chunk_view(owner, c):
        lo, hi = CHUNKS[c]
        return gathered.at[owner, pl.ds(lo * BLOCK, (hi - lo) * BLOCK)]

    bulk = []
    finish_sums(0, (0,))
    for c, (lo, hi) in enumerate(CHUNKS):
        if lo == PARTS[1][0]:
            finish_sums(1, (1, 2))
        for block in range(lo, hi):
            view = pl.ds(block * BLOCK, BLOCK)
            gathered[y, view, :] = (rows[view, :] * column(inverse, block)).astype(BF16)
        view = chunk_view(y, c)
        bulk.append(remote(view, view, up_send.at[c], up_recv.at[c], at_y(1)))
        bulk.append(remote(view, view, down_send.at[c], down_recv.at[c], at_y(3)))
        bulk[-2].start()
        bulk[-1].start()

    for copy in ry:
        copy.wait_recv()
    view = pieces.at[:, mine]
    rc = remote(view, view, rc_send, rc_recv, partner)
    rc.start()
    scales = [wide[p] for p in range(len(PARTS))]
    for block in range(12):
        same = lax.broadcasted_iota(jnp.int32, (BLOCK, 128), 0) == lax.broadcasted_iota(jnp.int32, (BLOCK, 128), 1)
        line = jnp.sum(jnp.where(same, column(scales, block), 0.0), axis=0, keepdims=True)
        scale_out[block // 6 : block // 6 + 1, (block % 6) * 128 : (block % 6 + 1) * 128] = line
    rc.wait_recv()
    view = pieces.at[:, pl.ds(z * 8 + x * 2, 2)]
    rx = [remote(view, view, rx_send.at[d - 1], rx_recv.at[d - 1], at_x(d)) for d in (1, 2, 3)]
    for copy in rx:
        copy.start()
    for copy in rx:
        copy.wait_recv()
    zu, zd = [], []
    for k in range(4):
        if k:
            zu[-1].wait_recv()
        view = pieces.at[:, pl.ds(lax.rem(z + nz - k, nz) * 8, 8)]
        zu.append(remote(view, view, zu_send.at[k], zu_recv.at[k], at_z(1)))
        zu[-1].start()
        if k < 3:
            if k:
                zd[-1].wait_recv()
            view = pieces.at[:, pl.ds(lax.rem(z + k, nz) * 8, 8)]
            zd.append(remote(view, view, zd_send.at[k], zd_recv.at[k], at_z(nz - 1)))
            zd[-1].start()

    forwards = []
    for k in range(HALF):
        bulk[2 * k].wait_recv()
        view = chunk_view(lax.rem(y + 3, ny), k)
        forwards.append(remote(view, view, fwd_up_send.at[k], fwd_up_recv.at[k], at_y(1)))
        forwards[-1].start()
        if k + HALF < len(CHUNKS):
            c = k + HALF
            bulk[2 * c + 1].wait_recv()
            view = chunk_view(lax.rem(y + 1, ny), c)
            forwards.append(remote(view, view, fwd_down_send.at[k], fwd_down_recv.at[k], at_y(3)))
            forwards[-1].start()

    zu[-1].wait_recv()
    zd[-1].wait_recv()

    def lay(step, _):
        for s in range(ny):
            four = [pieces[s, step * 4 + i].astype(F32) for i in range(4)]
            tall[pl.ds(pl.multiple_of(step * 8, 8), 8), s * 512 : (s + 1) * 512] = jnp.concatenate(four, axis=0)
        return 0

    lax.fori_loop(0, 16, lay, 0)
    for i in range(16):
        router_out[i * 128 : (i + 1) * 128, :] = tall[:, i * 128 : (i + 1) * 128].T.astype(BF16)

    for c in range(len(CHUNKS)):
        if c >= HALF:
            bulk[2 * c].wait_recv()
        else:
            bulk[2 * c + 1].wait_recv()
    for copy in forwards:
        copy.wait_recv()
    for copy in bulk + forwards + ry + [rc] + rx + zu + zd:
        copy.wait_send()
    for copies in sum_copies:
        for copy in copies:
            copy.wait_send()


def write_kernel(gathered, scale, router, down_out, scale_out, router_out, sems):
    copies = [
        pltpu.make_async_copy(gathered.at[s], down_out.at[:, pl.ds(s * 512, 512)], sems.at[s]) for s in range(4)
    ]
    copies.append(pltpu.make_async_copy(scale, scale_out, sems.at[4]))
    copies.append(pltpu.make_async_copy(router, router_out, sems.at[5]))
    for copy in copies:
        copy.start()
    for copy in copies:
        copy.wait()


def body(master_down, router_weight, router_gain):
    dma = pltpu.SemaphoreType.DMA
    n = len(CHUNKS)
    hbm = pl.BlockSpec(memory_space=pltpu.HBM)
    vmem = pl.BlockSpec(memory_space=pltpu.VMEM)
    gathered, scale, router = pl.pallas_call(
        gather_kernel,
        name="gather",
        out_shape=(
            pltpu.VMEM((4, 1536, 512), BF16),
            pltpu.VMEM((2, 768), F32),
            pltpu.VMEM((2048, 128), BF16),
        ),
        in_specs=[hbm] * 3,
        out_specs=[vmem] * 3,
        scratch_shapes=[
            pltpu.VMEM((1536, 512), F32),
            pltpu.VMEM((4, 3, 8, 128), F32),
            pltpu.VMEM((3, 8, 128), F32),
            pltpu.VMEM((2, 512), F32),
            pltpu.VMEM((1, 512), F32),
            pltpu.VMEM((4, 64, 2, 512), BF16),
            pltpu.VMEM((128, 2048), F32),
            dma((3,)), dma((2,)), dma((2, 3)), dma((2, 3)), dma((n,)), dma((n,)), dma((n,)), dma((n,)),
            dma((HALF,)), dma((HALF,)), dma((HALF,)), dma((HALF,)),
            dma((3,)), dma((3,)), dma(()), dma(()), dma((3,)), dma((3,)), dma((4,)), dma((4,)), dma((3,)), dma((3,)),
        ],
        compiler_params=pltpu.CompilerParams(collective_id=0, has_side_effects=True, vmem_limit_bytes=52 << 20),
    )(master_down.reshape(1536, 512), router_weight.T, router_gain.reshape(1, 512))
    down, scale, router = pl.pallas_call(
        write_kernel,
        name="write",
        out_shape=(
            jax.ShapeDtypeStruct((1536, 2048), BF16),
            jax.ShapeDtypeStruct((2, 768), F32),
            jax.ShapeDtypeStruct((2048, 128), BF16),
        ),
        in_specs=[vmem] * 3,
        out_specs=[hbm] * 3,
        scratch_shapes=[dma((6,))],
        compiler_params=pltpu.CompilerParams(vmem_limit_bytes=1 << 20),
    )(gathered, scale, router)
    return down.reshape(2, 768, 2048), scale, router


def solution(mesh):
    finer = Mesh(mesh.devices.reshape(8, 4, 2, mesh.shape["shard"]), (*EXPERT, "shard"))
    in_specs = (P(EXPERT, None, "shard"), P("shard", EXPERT), P("shard"))
    out_specs = (P(EXPERT, None, None), P(EXPERT, None), P())
    return jax.shard_map(body, mesh=finer, in_specs=in_specs, out_specs=out_specs, check_vma=False)
```

```python
import functools

import jax
import jax.numpy as jnp
from jax import lax
from jax.experimental import pallas as pl
from jax.experimental.pallas import tpu as pltpu
from jax.sharding import Mesh
from jax.sharding import PartitionSpec as P

MESH = pl.DeviceIdType.MESH
EXPERT = ("z", "x", "core")
BF16, F32 = jnp.bfloat16, jnp.float32

BLOCK = 128
GROUPS = BLOCK // 8
PARTS = ((0, 2), (2, 7), (7, 12))
CHUNKS = ((0, 1), (1, 2), (2, 4), (4, 6), (6, 8), (8, 10), (10, 12))
HALF = 4


def part_of(block):
    for p, (lo, hi) in enumerate(PARTS):
        if lo <= block < hi:
            return p, (block - lo) * GROUPS


def pick(first):
    lane = lax.broadcasted_iota(jnp.int32, (GROUPS, 8, 128), 2)
    group = lax.broadcasted_iota(jnp.int32, (GROUPS, 8, 128), 0)
    return lane == group + first


def column(packed, block):
    p, first = part_of(block)
    spread = jnp.where(pick(first), packed[p][None], 0.0)
    return jnp.sum(spread, axis=2, keepdims=True).reshape(BLOCK, 1)


def gather_kernel(
    master, router, gain,
    gathered, scale_out, router_out,
    rows, sums, wide, weight, gains, pieces, tall,
    load_sem, small_sem, sum_send, sum_recv, up_send, up_recv, down_send, down_recv,
    fwd_up_send, fwd_up_recv, fwd_down_send, fwd_down_recv,
    y_ready, far_ready, other_ready,
    ry_send, ry_recv, rc_send, rc_recv, rx_send, rx_recv, zu_send, zu_recv, zd_send, zd_recv,
):
    z, x, core, y = (lax.axis_index(a) for a in ("z", "x", "core", "shard"))
    nz, nx, ny = 8, 4, 4
    mine = z * (nx * 2) + x * 2 + core

    def at_y(step):
        return (z, x, core, lax.rem(y + step, ny))

    def at_x(step):
        return (z, lax.rem(x + step, nx), core, y)

    def at_z(step):
        return (lax.rem(z + step, nz), x, core, y)

    partner = (z, x, 1 - core, y)

    loads = []
    for p, (lo, hi) in enumerate(PARTS):
        view = pl.ds(lo * BLOCK, (hi - lo) * BLOCK)
        loads.append(pltpu.make_async_copy(master.at[view], rows.at[view], load_sem.at[p]))
        loads[-1].start()
    small = [
        pltpu.make_async_copy(router, weight, small_sem.at[0]),
        pltpu.make_async_copy(gain, gains, small_sem.at[1]),
    ]
    for copy in small:
        copy.start()

    barrier = pltpu.get_barrier_semaphore()
    even = lax.rem(x + y + z + core, 2) == 0
    odd = jnp.logical_not(even)
    beside = [at_y(1), at_y(ny - 1)]
    others = [at_z(1), at_z(nz - 1), at_x(1), at_x(nx - 1), partner]

    def tell(semaphore, peers):
        for peer in peers:
            pl.semaphore_signal(semaphore, inc=1, device_id=peer, device_id_type=MESH)

    @pl.when(even)
    def _():
        tell(barrier, others)
        pl.semaphore_wait(barrier, len(beside))
        tell(y_ready, beside)

    @pl.when(odd)
    def _():
        tell(barrier, beside)
        pl.semaphore_wait(y_ready, len(beside))
        tell(far_ready, beside[1:])

    def remote(src, dst, send, recv, peer):
        copy = pltpu.make_async_remote_copy(
            src_ref=src, dst_ref=dst, send_sem=send, recv_sem=recv, device_id=peer, device_id_type=MESH
        )
        return copy

    def partial_sums(p):
        lo, hi = PARTS[p]
        loads[p].wait()
        packed = jnp.zeros((8, 128), F32)
        for block in range(lo, hi):
            values = rows[pl.ds(block * BLOCK, BLOCK), :]
            total = jnp.sum(values * values, axis=1, keepdims=True).reshape(GROUPS, 8, 1)
            packed = packed + jnp.sum(jnp.where(pick((block - lo) * GROUPS), total, 0.0), axis=0)
        sums[y, p] = packed

    def send_sums(first, count, slot):
        out = []
        for d in (1, 3, 2):
            if d == 2 and slot == 0:

                @pl.when(even)
                def _():
                    pl.semaphore_wait(far_ready, 1)

            view = sums.at[y, pl.ds(first, count)]
            out.append(remote(view, view, sum_send.at[slot, d - 1], sum_recv.at[slot, d - 1], at_y(d)))
            out[-1].start()
        return out

    partial_sums(0)
    for copy in small:
        copy.wait()
    pieces[y, mine] = (weight[...] * gains[...]).astype(BF16)
    sum_copies = [send_sums(0, 1, 0)]
    partial_sums(1)
    partial_sums(2)
    sum_copies.append(send_sums(1, 2, 1))

    view = pieces.at[y, mine]
    ry = [remote(view, view, ry_send.at[d - 1], ry_recv.at[d - 1], at_y(d)) for d in (1, 2, 3)]
    for copy in ry:
        copy.start()

    inverse = {}

    def finish_sums(slot, parts):
        for copy in sum_copies[slot]:
            copy.wait_recv()
        for p in parts:
            scale = jnp.sqrt((sums[0, p] + sums[1, p]) + (sums[2, p] + sums[3, p]))
            wide[p] = scale
            inverse[p] = 1.0 / scale

    def chunk_view(owner, c):
        lo, hi = CHUNKS[c]
        return gathered.at[owner, pl.ds(lo * BLOCK, (hi - lo) * BLOCK)]

    bulk = []
    finish_sums(0, (0,))
    for c, (lo, hi) in enumerate(CHUNKS):
        if lo == PARTS[1][0]:
            finish_sums(1, (1, 2))
        for block in range(lo, hi):
            view = pl.ds(block * BLOCK, BLOCK)
            gathered[y, view, :] = (rows[view, :] * column(inverse, block)).astype(BF16)
        view = chunk_view(y, c)
        bulk.append(remote(view, view, up_send.at[c], up_recv.at[c], at_y(1)))
        bulk.append(remote(view, view, down_send.at[c], down_recv.at[c], at_y(3)))
        bulk[-2].start()
        bulk[-1].start()

    for copy in ry:
        copy.wait_recv()
    view = pieces.at[:, mine]

    @pl.when(even)
    def _():
        pl.semaphore_wait(other_ready, len(others))

    @pl.when(odd)
    def _():
        pl.semaphore_wait(barrier, len(others))
        tell(other_ready, others)

    rc = remote(view, view, rc_send, rc_recv, partner)
    rc.start()
    scales = [wide[p] for p in range(len(PARTS))]
    for block in range(12):
        same = lax.broadcasted_iota(jnp.int32, (BLOCK, 128), 0) == lax.broadcasted_iota(jnp.int32, (BLOCK, 128), 1)
        line = jnp.sum(jnp.where(same, column(scales, block), 0.0), axis=0, keepdims=True)
        scale_out[block // 6 : block // 6 + 1, (block % 6) * 128 : (block % 6 + 1) * 128] = line
    rc.wait_recv()
    view = pieces.at[:, pl.ds(z * 8 + x * 2, 2)]
    rx = [remote(view, view, rx_send.at[k], rx_recv.at[k], at_x((1, nx - 1)[k])) for k in range(2)]
    for copy in rx:
        copy.start()
    rx[0].wait_recv()
    view = pieces.at[:, pl.ds(z * 8 + lax.rem(x + nx - 1, nx) * 2, 2)]
    rx.append(remote(view, view, rx_send.at[2], rx_recv.at[2], at_x(1)))
    rx[2].start()
    rx[1].wait_recv()
    rx[2].wait_recv()
    zu, zd = [], []
    for k in range(4):
        if k:
            zu[-1].wait_recv()
        view = pieces.at[:, pl.ds(lax.rem(z + nz - k, nz) * 8, 8)]
        zu.append(remote(view, view, zu_send.at[k], zu_recv.at[k], at_z(1)))
        zu[-1].start()
        if k < 3:
            if k:
                zd[-1].wait_recv()
            view = pieces.at[:, pl.ds(lax.rem(z + k, nz) * 8, 8)]
            zd.append(remote(view, view, zd_send.at[k], zd_recv.at[k], at_z(nz - 1)))
            zd[-1].start()

    forwards = []
    for k in range(HALF):
        bulk[2 * k].wait_recv()
        view = chunk_view(lax.rem(y + 3, ny), k)
        forwards.append(remote(view, view, fwd_up_send.at[k], fwd_up_recv.at[k], at_y(1)))
        forwards[-1].start()
        if k + HALF < len(CHUNKS):
            c = k + HALF
            bulk[2 * c + 1].wait_recv()
            view = chunk_view(lax.rem(y + 1, ny), c)
            forwards.append(remote(view, view, fwd_down_send.at[k], fwd_down_recv.at[k], at_y(3)))
            forwards[-1].start()

    zu[-1].wait_recv()
    zd[-1].wait_recv()

    def lay(step, _):
        for s in range(ny):
            four = [pieces[s, step * 4 + i].astype(F32) for i in range(4)]
            tall[pl.ds(pl.multiple_of(step * 8, 8), 8), s * 512 : (s + 1) * 512] = jnp.concatenate(four, axis=0)
        return 0

    lax.fori_loop(0, 16, lay, 0)
    for i in range(16):
        router_out[i * 128 : (i + 1) * 128, :] = tall[:, i * 128 : (i + 1) * 128].T.astype(BF16)

    for c in range(len(CHUNKS)):
        if c >= HALF:
            bulk[2 * c].wait_recv()
        else:
            bulk[2 * c + 1].wait_recv()
    for copy in forwards:
        copy.wait_recv()
    for copy in bulk + forwards + ry + [rc] + rx + zu + zd:
        copy.wait_send()
    for copies in sum_copies:
        for copy in copies:
            copy.wait_send()


def write_kernel(gathered, scale, router, down_out, scale_out, router_out, sems):
    copies = [
        pltpu.make_async_copy(
            gathered.at[s, pl.ds(r * 384, 384)], down_out.at[pl.ds(r * 384, 384), pl.ds(s * 512, 512)], sems.at[s, r]
        )
        for r in range(4)
        for s in range(4)
    ]
    copies.append(pltpu.make_async_copy(scale, scale_out, sems.at[4, 0]))
    copies.append(pltpu.make_async_copy(router, router_out, sems.at[4, 1]))
    for copy in copies:
        copy.start()
    for copy in copies:
        copy.wait()


def body(master_down, router_weight, router_gain):
    dma, regular = pltpu.SemaphoreType.DMA, pltpu.SemaphoreType.REGULAR
    n = len(CHUNKS)
    hbm = pl.BlockSpec(memory_space=pltpu.HBM)
    vmem = pl.BlockSpec(memory_space=pltpu.VMEM)
    gathered, scale, router = pl.pallas_call(
        gather_kernel,
        name="gather",
        out_shape=(
            pltpu.VMEM((4, 1536, 512), BF16),
            pltpu.VMEM((2, 768), F32),
            pltpu.VMEM((2048, 128), BF16),
        ),
        in_specs=[hbm] * 3,
        out_specs=[vmem] * 3,
        scratch_shapes=[
            pltpu.VMEM((1536, 512), F32),
            pltpu.VMEM((4, 3, 8, 128), F32),
            pltpu.VMEM((3, 8, 128), F32),
            pltpu.VMEM((2, 512), F32),
            pltpu.VMEM((1, 512), F32),
            pltpu.VMEM((4, 64, 2, 512), BF16),
            pltpu.VMEM((128, 2048), F32),
            dma((3,)), dma((2,)), dma((2, 3)), dma((2, 3)), dma((n,)), dma((n,)), dma((n,)), dma((n,)),
            dma((HALF,)), dma((HALF,)), dma((HALF,)), dma((HALF,)),
            regular, regular, regular,
            dma((3,)), dma((3,)), dma(()), dma(()), dma((3,)), dma((3,)), dma((4,)), dma((4,)), dma((3,)), dma((3,)),
        ],
        compiler_params=pltpu.CompilerParams(collective_id=0, has_side_effects=True, vmem_limit_bytes=52 << 20),
    )(master_down.reshape(1536, 512), router_weight.T, router_gain.reshape(1, 512))
    down, scale, router = pl.pallas_call(
        write_kernel,
        name="write",
        out_shape=(
            jax.ShapeDtypeStruct((1536, 2048), BF16),
            jax.ShapeDtypeStruct((2, 768), F32),
            jax.ShapeDtypeStruct((2048, 128), BF16),
        ),
        in_specs=[vmem] * 3,
        out_specs=[hbm] * 3,
        scratch_shapes=[dma((5, 4))],
        compiler_params=pltpu.CompilerParams(vmem_limit_bytes=1 << 20),
    )(gathered, scale, router)
    return down.reshape(2, 768, 2048), scale, router


def solution(mesh):
    finer = Mesh(mesh.devices.reshape(8, 4, 2, mesh.shape["shard"]), (*EXPERT, "shard"))
    in_specs = (P(EXPERT, None, "shard"), P("shard", EXPERT), P("shard"))
    out_specs = (P(EXPERT, None, None), P(EXPERT, None), P())
    return jax.shard_map(body, mesh=finer, in_specs=in_specs, out_specs=out_specs, check_vma=False)
```

```python
import functools

import jax
import jax.numpy as jnp
from jax import lax
from jax.experimental import pallas as pl
from jax.experimental.pallas import tpu as pltpu
from jax.sharding import Mesh
from jax.sharding import PartitionSpec as P

MESH = pl.DeviceIdType.MESH
EXPERT = ("z", "x", "core")
BF16, F32 = jnp.bfloat16, jnp.float32

BLOCK = 128
GROUPS = BLOCK // 8
PARTS = ((0, 2), (2, 7), (7, 12))
CHUNKS = ((0, 1), (1, 2), (2, 4), (4, 6), (6, 8), (8, 10), (10, 12))
HALF = 4


def part_of(block):
    for p, (lo, hi) in enumerate(PARTS):
        if lo <= block < hi:
            return p, (block - lo) * GROUPS


def pick(first):
    lane = lax.broadcasted_iota(jnp.int32, (GROUPS, 8, 128), 2)
    group = lax.broadcasted_iota(jnp.int32, (GROUPS, 8, 128), 0)
    return lane == group + first


def column(packed, block):
    p, first = part_of(block)
    spread = jnp.where(pick(first), packed[p][None], 0.0)
    return jnp.sum(spread, axis=2, keepdims=True).reshape(BLOCK, 1)


def gather_kernel(
    master, router, gain,
    gathered, scale_out, router_out,
    rows, sums, wide, weight, gains, pieces, tall,
    load_sem, small_sem, sum_send, sum_recv, up_send, up_recv, down_send, down_recv,
    fwd_up_send, fwd_up_recv, fwd_down_send, fwd_down_recv,
    group_ready, other_ready,
    ry_send, ry_recv, rc_send, rc_recv, rx_send, rx_recv, zu_send, zu_recv, zd_send, zd_recv,
):
    z, x, core, y = (lax.axis_index(a) for a in ("z", "x", "core", "shard"))
    nz, nx, ny = 8, 4, 4
    mine = z * (nx * 2) + x * 2 + core

    def at_y(step):
        return (z, x, core, lax.rem(y + step, ny))

    def at_x(step):
        return (z, lax.rem(x + step, nx), core, y)

    def at_z(step):
        return (lax.rem(z + step, nz), x, core, y)

    partner = (z, x, 1 - core, y)

    loads = []
    for p, (lo, hi) in enumerate(PARTS):
        view = pl.ds(lo * BLOCK, (hi - lo) * BLOCK)
        loads.append(pltpu.make_async_copy(master.at[view], rows.at[view], load_sem.at[p]))
        loads[-1].start()
    small = [
        pltpu.make_async_copy(router, weight, small_sem.at[0]),
        pltpu.make_async_copy(gain, gains, small_sem.at[1]),
    ]
    for copy in small:
        copy.start()

    barrier = pltpu.get_barrier_semaphore()
    gateway = y == ny - 1
    ordinary = y < ny - 1
    others = [at_z(1), at_z(nz - 1), at_x(1), at_x(nx - 1), partner]

    def tell(semaphore, peers):
        for peer in peers:
            pl.semaphore_signal(semaphore, inc=1, device_id=peer, device_id_type=MESH)

    for d in (1, 2, 3):

        @pl.when(y + d != ny - 1)
        def _(d=d):
            tell(barrier, [at_y(d)])

    def remote(src, dst, send, recv, peer):
        copy = pltpu.make_async_remote_copy(
            src_ref=src, dst_ref=dst, send_sem=send, recv_sem=recv, device_id=peer, device_id_type=MESH
        )
        return copy

    def partial_sums(p):
        lo, hi = PARTS[p]
        loads[p].wait()
        packed = jnp.zeros((8, 128), F32)
        for block in range(lo, hi):
            values = rows[pl.ds(block * BLOCK, BLOCK), :]
            total = jnp.sum(values * values, axis=1, keepdims=True).reshape(GROUPS, 8, 1)
            packed = packed + jnp.sum(jnp.where(pick((block - lo) * GROUPS), total, 0.0), axis=0)
        sums[y, p] = packed

    def send_sums(first, count, slot):
        out = []
        for d in (1, 3, 2):
            view = sums.at[y, pl.ds(first, count)]
            out.append(remote(view, view, sum_send.at[slot, d - 1], sum_recv.at[slot, d - 1], at_y(d)))
            out[-1].start()
        return out

    partial_sums(0)
    for copy in small:
        copy.wait()
    pieces[y, mine] = (weight[...] * gains[...]).astype(BF16)

    @pl.when(ordinary)
    def _():
        pl.semaphore_wait(barrier, ny - 1)

    @pl.when(y == 0)
    def _():
        tell(group_ready, [at_y(ny - 1)])

    @pl.when(gateway)
    def _():
        pl.semaphore_wait(group_ready, 1)
        tell(barrier, others)

    sum_copies = [send_sums(0, 1, 0)]
    partial_sums(1)
    partial_sums(2)
    sum_copies.append(send_sums(1, 2, 1))

    view = pieces.at[y, mine]
    ry = [remote(view, view, ry_send.at[d - 1], ry_recv.at[d - 1], at_y(d)) for d in (1, 2, 3)]
    for copy in ry:
        copy.start()

    inverse = {}

    def finish_sums(slot, parts):
        for copy in sum_copies[slot]:
            copy.wait_recv()
        for p in parts:
            scale = jnp.sqrt((sums[0, p] + sums[1, p]) + (sums[2, p] + sums[3, p]))
            wide[p] = scale
            inverse[p] = 1.0 / scale

    def chunk_view(owner, c):
        lo, hi = CHUNKS[c]
        return gathered.at[owner, pl.ds(lo * BLOCK, (hi - lo) * BLOCK)]

    bulk = []
    finish_sums(0, (0,))
    for c, (lo, hi) in enumerate(CHUNKS):
        if lo == PARTS[1][0]:
            finish_sums(1, (1, 2))
        for block in range(lo, hi):
            view = pl.ds(block * BLOCK, BLOCK)
            gathered[y, view, :] = (rows[view, :] * column(inverse, block)).astype(BF16)
        view = chunk_view(y, c)
        bulk.append(remote(view, view, up_send.at[c], up_recv.at[c], at_y(1)))
        bulk.append(remote(view, view, down_send.at[c], down_recv.at[c], at_y(3)))
        bulk[-2].start()
        bulk[-1].start()

    for copy in ry:
        copy.wait_recv()
    view = pieces.at[:, mine]

    @pl.when(gateway)
    def _():
        pl.semaphore_wait(barrier, len(others))
        tell(other_ready, [at_y(d) for d in (1, 2, 3)])

    @pl.when(ordinary)
    def _():
        pl.semaphore_wait(other_ready, 1)

    rc = remote(view, view, rc_send, rc_recv, partner)
    rc.start()
    scales = [wide[p] for p in range(len(PARTS))]
    for block in range(12):
        same = lax.broadcasted_iota(jnp.int32, (BLOCK, 128), 0) == lax.broadcasted_iota(jnp.int32, (BLOCK, 128), 1)
        line = jnp.sum(jnp.where(same, column(scales, block), 0.0), axis=0, keepdims=True)
        scale_out[block // 6 : block // 6 + 1, (block % 6) * 128 : (block % 6 + 1) * 128] = line
    rc.wait_recv()
    view = pieces.at[:, pl.ds(z * 8 + x * 2, 2)]
    rx = [remote(view, view, rx_send.at[k], rx_recv.at[k], at_x((1, nx - 1)[k])) for k in range(2)]
    for copy in rx:
        copy.start()
    rx[0].wait_recv()
    view = pieces.at[:, pl.ds(z * 8 + lax.rem(x + nx - 1, nx) * 2, 2)]
    rx.append(remote(view, view, rx_send.at[2], rx_recv.at[2], at_x(1)))
    rx[2].start()
    rx[1].wait_recv()
    rx[2].wait_recv()
    zu, zd = [], []
    for k in range(4):
        if k:
            zu[-1].wait_recv()
        view = pieces.at[:, pl.ds(lax.rem(z + nz - k, nz) * 8, 8)]
        zu.append(remote(view, view, zu_send.at[k], zu_recv.at[k], at_z(1)))
        zu[-1].start()
        if k < 3:
            if k:
                zd[-1].wait_recv()
            view = pieces.at[:, pl.ds(lax.rem(z + k, nz) * 8, 8)]
            zd.append(remote(view, view, zd_send.at[k], zd_recv.at[k], at_z(nz - 1)))
            zd[-1].start()

    forwards = []
    for k in range(HALF):
        bulk[2 * k].wait_recv()
        view = chunk_view(lax.rem(y + 3, ny), k)
        forwards.append(remote(view, view, fwd_up_send.at[k], fwd_up_recv.at[k], at_y(1)))
        forwards[-1].start()
        if k + HALF < len(CHUNKS):
            c = k + HALF
            bulk[2 * c + 1].wait_recv()
            view = chunk_view(lax.rem(y + 1, ny), c)
            forwards.append(remote(view, view, fwd_down_send.at[k], fwd_down_recv.at[k], at_y(3)))
            forwards[-1].start()

    zu[-1].wait_recv()
    zd[-1].wait_recv()

    def lay(step, _):
        for s in range(ny):
            four = [pieces[s, step * 4 + i].astype(F32) for i in range(4)]
            tall[pl.ds(pl.multiple_of(step * 8, 8), 8), s * 512 : (s + 1) * 512] = jnp.concatenate(four, axis=0)
        return 0

    lax.fori_loop(0, 16, lay, 0)
    for i in range(16):
        router_out[i * 128 : (i + 1) * 128, :] = tall[:, i * 128 : (i + 1) * 128].T.astype(BF16)

    for c in range(len(CHUNKS)):
        if c >= HALF:
            bulk[2 * c].wait_recv()
        else:
            bulk[2 * c + 1].wait_recv()
    for copy in forwards:
        copy.wait_recv()
    for copy in bulk + forwards + ry + [rc] + rx + zu + zd:
        copy.wait_send()
    for copies in sum_copies:
        for copy in copies:
            copy.wait_send()


def write_kernel(gathered, scale, router, down_out, scale_out, router_out, sems):
    copies = [
        pltpu.make_async_copy(
            gathered.at[s, pl.ds(r * 768, 768)], down_out.at[pl.ds(r * 768, 768), pl.ds(s * 512, 512)], sems.at[s, r]
        )
        for r in range(2)
        for s in range(4)
    ]
    copies.append(pltpu.make_async_copy(scale, scale_out, sems.at[4, 0]))
    copies.append(pltpu.make_async_copy(router, router_out, sems.at[4, 1]))
    for copy in copies:
        copy.start()
    for copy in copies:
        copy.wait()


def body(master_down, router_weight, router_gain):
    dma, regular = pltpu.SemaphoreType.DMA, pltpu.SemaphoreType.REGULAR
    n = len(CHUNKS)
    hbm = pl.BlockSpec(memory_space=pltpu.HBM)
    vmem = pl.BlockSpec(memory_space=pltpu.VMEM)
    gathered, scale, router = pl.pallas_call(
        gather_kernel,
        name="gather",
        out_shape=(
            pltpu.VMEM((4, 1536, 512), BF16),
            pltpu.VMEM((2, 768), F32),
            pltpu.VMEM((2048, 128), BF16),
        ),
        in_specs=[hbm] * 3,
        out_specs=[vmem] * 3,
        scratch_shapes=[
            pltpu.VMEM((1536, 512), F32),
            pltpu.VMEM((4, 3, 8, 128), F32),
            pltpu.VMEM((3, 8, 128), F32),
            pltpu.VMEM((2, 512), F32),
            pltpu.VMEM((1, 512), F32),
            pltpu.VMEM((4, 64, 2, 512), BF16),
            pltpu.VMEM((128, 2048), F32),
            dma((3,)), dma((2,)), dma((2, 3)), dma((2, 3)), dma((n,)), dma((n,)), dma((n,)), dma((n,)),
            dma((HALF,)), dma((HALF,)), dma((HALF,)), dma((HALF,)),
            regular, regular,
            dma((3,)), dma((3,)), dma(()), dma(()), dma((3,)), dma((3,)), dma((4,)), dma((4,)), dma((3,)), dma((3,)),
        ],
        compiler_params=pltpu.CompilerParams(collective_id=0, has_side_effects=True, vmem_limit_bytes=52 << 20),
    )(master_down.reshape(1536, 512), router_weight.T, router_gain.reshape(1, 512))
    down, scale, router = pl.pallas_call(
        write_kernel,
        name="write",
        out_shape=(
            jax.ShapeDtypeStruct((1536, 2048), BF16),
            jax.ShapeDtypeStruct((2, 768), F32),
            jax.ShapeDtypeStruct((2048, 128), BF16),
        ),
        in_specs=[vmem] * 3,
        out_specs=[hbm] * 3,
        scratch_shapes=[dma((5, 4))],
        compiler_params=pltpu.CompilerParams(vmem_limit_bytes=1 << 20),
    )(gathered, scale, router)
    return down.reshape(2, 768, 2048), scale, router


def solution(mesh):
    finer = Mesh(mesh.devices.reshape(8, 4, 2, mesh.shape["shard"]), (*EXPERT, "shard"))
    in_specs = (P(EXPERT, None, "shard"), P("shard", EXPERT), P("shard"))
    out_specs = (P(EXPERT, None, None), P(EXPERT, None), P())
    return jax.shard_map(body, mesh=finer, in_specs=in_specs, out_specs=out_specs, check_vma=False)
```

```python
import jax
import jax.numpy as jnp
from jax import lax
from jax.experimental import pallas as pl
from jax.experimental.pallas import tpu as pltpu
from jax.sharding import Mesh
from jax.sharding import PartitionSpec as P

MESH = pl.DeviceIdType.MESH
EXPERT = ("z", "x", "core")
BF16, F32 = jnp.bfloat16, jnp.float32

BLOCK = 128
GROUPS = BLOCK // 8
PARTS = ((0, 2), (2, 7), (7, 12))
CHUNKS = ((0, 1), (1, 2), (2, 6), (6, 12))
UP_ORDER, DOWN_ORDER = (0, 1, 2, 3), (0, 1, 3, 2)
HALF = 768
RAW = 48


def part_of(block):
    for p, (lo, hi) in enumerate(PARTS):
        if lo <= block < hi:
            return p, (block - lo) * GROUPS


def pick(first):
    lane = lax.broadcasted_iota(jnp.int32, (GROUPS, 8, 128), 2)
    group = lax.broadcasted_iota(jnp.int32, (GROUPS, 8, 128), 0)
    return lane == group + first


def column(packed, block):
    p, first = part_of(block)
    spread = jnp.where(pick(first), packed[p][None], 0.0)
    return jnp.sum(spread, axis=2, keepdims=True).reshape(BLOCK, 1)


def done(view, semaphore):
    pltpu.make_async_copy(view, view, semaphore).wait()


def gather_kernel(
    master, router, gain,
    gathered, scale_out, router_out,
    rows, raw, sums, wide, weight, gains, pieces, tall,
    load_sem, small_sem, sum_send, sum_recv, raw_send, raw_recv,
    up_send, down_send, up_recv, down_recv, group_ready, other_ready,
    row_send, row_recv, col_send, rc_recv, rx_recv, zu_recv, zd_recv,
):
    z, x, core, y = (lax.axis_index(a) for a in ("z", "x", "core", "shard"))
    nz, nx, ny = 8, 4, 4
    mine = z * (nx * 2) + x * 2 + core
    below, above = lax.rem(y + ny - 1, ny), lax.rem(y + 1, ny)
    first_raw = 12 * BLOCK - RAW

    def at_y(step):
        return (z, x, core, lax.rem(y + step, ny))

    def at_x(step):
        return (z, lax.rem(x + step, nx), core, y)

    def at_z(step):
        return (lax.rem(z + step, nz), x, core, y)

    partner = (z, x, 1 - core, y)

    def tell(semaphore, peers):
        for peer in peers:
            pl.semaphore_signal(semaphore, inc=1, device_id=peer, device_id_type=MESH)

    def send(src, dst, send_sem, recv_sem, peer):
        pltpu.make_async_remote_copy(
            src_ref=src, dst_ref=dst, send_sem=send_sem, recv_sem=recv_sem, device_id=peer, device_id_type=MESH
        ).start()

    barrier = pltpu.get_barrier_semaphore()
    gateway = y == ny - 1
    ordinary = y < ny - 1
    others = [at_z(1), at_z(nz - 1), at_x(1), at_x(nx - 1), partner]
    for d in (1, 3, 2):

        @pl.when(y + d != ny - 1)
        def _(d=d):
            tell(barrier, [at_y(d)])

    def load(at, count, k):
        view = pl.ds(at, count)
        return pltpu.make_async_copy(master.at[view], rows.at[view], load_sem.at[k])

    small = [
        pltpu.make_async_copy(router, weight, small_sem.at[0]),
        pltpu.make_async_copy(gain, gains, small_sem.at[1]),
    ]
    loads = [load(0, 256, 0), load(first_raw, RAW, 1), load(256, first_raw - 256, 2)]
    loads[0].start()
    loads[1].start()
    for copy in small:
        copy.start()
    loads[2].start()

    @pl.when(ordinary)
    def _():
        pl.semaphore_wait(barrier, ny - 1)

    @pl.when(y == ny - 2)
    def _():
        tell(group_ready, [at_y(1)])

    def partial_sums(p):
        lo, hi = PARTS[p]
        packed = jnp.zeros((8, 128), F32)
        for block in range(lo, hi):
            values = rows[pl.ds(block * BLOCK, BLOCK), :]
            total = jnp.sum(values * values, axis=1, keepdims=True).reshape(GROUPS, 8, 1)
            packed = packed + jnp.sum(jnp.where(pick((block - lo) * GROUPS), total, 0.0), axis=0)
        sums[y, p] = packed

    def send_sums(first, count, slot):
        view = sums.at[y, pl.ds(first, count)]
        for d in (2, 1, 3):
            send(view, view, sum_send, sum_recv.at[slot], at_y(d))

    loads[0].wait()
    partial_sums(0)

    @pl.when(gateway)
    def _():
        pl.semaphore_wait(group_ready, 1)

    send_sums(0, 1, 0)
    loads[1].wait()
    view = rows.at[pl.ds(first_raw, RAW)]
    send(view, raw.at[0], raw_send, raw_recv, at_y(1))
    send(view, raw.at[1], raw_send, raw_recv, at_y(ny - 1))

    @pl.when(gateway)
    def _():
        tell(barrier, others)

    loads[2].wait()
    partial_sums(1)
    partial_sums(2)
    send_sums(1, 2, 1)

    for copy in small:
        copy.wait()
    pieces[y, mine] = (weight[...] * gains[...]).astype(BF16)
    view = pieces.at[y, mine]
    for d in (1, 2, 3):
        send(view, view, row_send, row_recv, at_y(d))

    inverse = {}

    def finish_sums(slot, parts):
        done(sums.at[pl.ds(0, ny - 1), pl.ds(parts[0], len(parts))], sum_recv.at[slot])
        for p in parts:
            scale = jnp.sqrt((sums[0, p] + sums[1, p]) + (sums[2, p] + sums[3, p]))
            wide[p] = scale
            inverse[p] = 1.0 / scale

    def rescale(c):
        for block in range(*CHUNKS[c]):
            view = pl.ds(block * BLOCK, BLOCK)
            gathered[y, view, :] = (rows[view, :] * column(inverse, block)).astype(BF16)

    def send_chunk(c, upwards):
        lo, hi = CHUNKS[c][0] * BLOCK, min(CHUNKS[c][1] * BLOCK, first_raw)
        view = gathered.at[y, pl.ds(lo, hi - lo)]
        onwards = (hi <= HALF) == upwards
        k = 0 if onwards else 1
        if upwards:
            send(view, view, up_send, up_recv.at[k], at_y(1))
        else:
            send(view, view, down_send, down_recv.at[k], at_y(ny - 1))

    finish_sums(0, (0,))
    for c in (0, 1):
        rescale(c)
        send_chunk(c, True)
        send_chunk(c, False)
    finish_sums(1, (1, 2))
    rescale(2)
    send_chunk(2, True)
    rescale(3)
    send_chunk(3, False)
    send_chunk(3, True)
    send_chunk(2, False)

    done(raw, raw_recv)
    last = column(inverse, 11)[BLOCK - RAW :]
    for k, owner in enumerate((below, above)):
        gathered[owner, pl.ds(first_raw, RAW), :] = (raw[k] * last).astype(BF16)

    done(pieces.at[pl.ds(0, ny - 1), 0], row_recv)
    scales = [wide[p] for p in range(len(PARTS))]
    for block in range(12):
        same = lax.broadcasted_iota(jnp.int32, (BLOCK, 128), 0) == lax.broadcasted_iota(jnp.int32, (BLOCK, 128), 1)
        line = jnp.sum(jnp.where(same, column(scales, block), 0.0), axis=0, keepdims=True)
        scale_out[block // 6 : block // 6 + 1, (block % 6) * 128 : (block % 6 + 1) * 128] = line

    @pl.when(gateway)
    def _():
        pl.semaphore_wait(barrier, len(others))
        tell(other_ready, [at_y(d) for d in (1, 2, 3)])

    @pl.when(ordinary)
    def _():
        pl.semaphore_wait(other_ready, 1)

    view = pieces.at[:, mine]
    send(view, view, col_send, rc_recv, partner)
    done(view, rc_recv)
    view = pieces.at[:, pl.ds(z * 8 + x * 2, 2)]
    send(view, view, col_send, rx_recv.at[0], at_x(1))
    send(view, view, col_send, rx_recv.at[1], at_x(nx - 1))
    done(view, rx_recv.at[0])
    view = pieces.at[:, pl.ds(z * 8 + lax.rem(x + nx - 1, nx) * 2, 2)]
    send(view, view, col_send, rx_recv.at[1], at_x(1))
    done(pieces.at[:, pl.ds(0, 4)], rx_recv.at[1])

    def plane(step):
        return pieces.at[:, pl.ds(lax.rem(z + step, nz) * 8, 8)]

    for k in range(4):
        if k:
            done(plane(0), zu_recv.at[k - 1])
        send(plane(nz - k), plane(nz - k), col_send, zu_recv.at[k], at_z(1))
        if k < 3:
            if k:
                done(plane(0), zd_recv.at[k - 1])
            send(plane(k), plane(k), col_send, zd_recv.at[k], at_z(nz - 1))

    view = gathered.at[below, pl.ds(0, HALF)]
    done(view, up_recv.at[0])
    send(view, view, up_send, up_recv.at[2], at_y(1))
    view = gathered.at[above, pl.ds(HALF, 12 * BLOCK - HALF)]
    done(gathered.at[0, pl.ds(0, first_raw - HALF)], down_recv.at[0])
    send(view, view, down_send, down_recv.at[2], at_y(ny - 1))

    done(plane(0), zu_recv.at[3])
    done(plane(0), zd_recv.at[2])

    def lay(step, _):
        for s in range(ny):
            four = [pieces[s, step * 4 + i].astype(F32) for i in range(4)]
            tall[pl.ds(pl.multiple_of(step * 8, 8), 8), s * 512 : (s + 1) * 512] = jnp.concatenate(four, axis=0)
        return 0

    lax.fori_loop(0, 16, lay, 0)
    for i in range(16):
        router_out[i * 128 : (i + 1) * 128, :] = tall[:, i * 128 : (i + 1) * 128].T.astype(BF16)

    done(sums.at[pl.ds(0, ny - 1)], sum_send)
    done(raw, raw_send)
    done(pieces.at[pl.ds(0, ny - 1), 0], row_send)
    done(pieces.at[:, pl.ds(0, 63)], col_send)
    done(gathered.at[0, pl.ds(0, first_raw - HALF)], up_recv.at[1])
    done(gathered.at[0, pl.ds(0, HALF)], down_recv.at[1])
    sent = gathered.at[pl.ds(0, 2), pl.ds(0, (first_raw + HALF) // 2)]
    done(sent, up_send)
    done(sent, down_send)
    done(gathered.at[0, pl.ds(0, HALF)], up_recv.at[2])
    done(gathered.at[0, pl.ds(0, 12 * BLOCK - HALF)], down_recv.at[2])


def write_kernel(gathered, scale, router, down_out, scale_out, router_out, sems):
    copies = [
        pltpu.make_async_copy(gathered.at[s], down_out.at[:, pl.ds(s * 512, 512)], sems.at[0]) for s in range(4)
    ]
    copies.append(pltpu.make_async_copy(scale, scale_out, sems.at[1]))
    copies.append(pltpu.make_async_copy(router, router_out, sems.at[2]))
    for copy in copies:
        copy.start()
    done(down_out, sems.at[0])
    copies[4].wait()
    copies[5].wait()


def body(master_down, router_weight, router_gain):
    dma, regular = pltpu.SemaphoreType.DMA, pltpu.SemaphoreType.REGULAR
    hbm = pl.BlockSpec(memory_space=pltpu.HBM)
    vmem = pl.BlockSpec(memory_space=pltpu.VMEM)
    gathered, scale, router = pl.pallas_call(
        gather_kernel,
        name="gather",
        out_shape=(
            pltpu.VMEM((4, 1536, 512), BF16),
            pltpu.VMEM((2, 768), F32),
            pltpu.VMEM((2048, 128), BF16),
        ),
        in_specs=[hbm] * 3,
        out_specs=[vmem] * 3,
        scratch_shapes=[
            pltpu.VMEM((1536, 512), F32),
            pltpu.VMEM((2, RAW, 512), F32),
            pltpu.VMEM((4, 3, 8, 128), F32),
            pltpu.VMEM((3, 8, 128), F32),
            pltpu.VMEM((2, 512), F32),
            pltpu.VMEM((1, 512), F32),
            pltpu.VMEM((4, 64, 2, 512), BF16),
            pltpu.VMEM((128, 2048), F32),
            dma((3,)), dma((2,)), dma(()), dma((2,)), dma(()), dma(()),
            dma(()), dma(()), dma((3,)), dma((3,)), regular, regular,
            dma(()), dma(()), dma(()), dma(()), dma((2,)), dma((4,)), dma((3,)),
        ],
        compiler_params=pltpu.CompilerParams(collective_id=0, has_side_effects=True, vmem_limit_bytes=52 << 20),
    )(master_down.reshape(1536, 512), router_weight.T, router_gain.reshape(1, 512))
    down, scale, router = pl.pallas_call(
        write_kernel,
        name="write",
        out_shape=(
            jax.ShapeDtypeStruct((1536, 2048), BF16),
            jax.ShapeDtypeStruct((2, 768), F32),
            jax.ShapeDtypeStruct((2048, 128), BF16),
        ),
        in_specs=[vmem] * 3,
        out_specs=[hbm] * 3,
        scratch_shapes=[dma((3,))],
        compiler_params=pltpu.CompilerParams(vmem_limit_bytes=1 << 20),
    )(gathered, scale, router)
    return down.reshape(2, 768, 2048), scale, router


def solution(mesh):
    finer = Mesh(mesh.devices.reshape(8, 4, 2, mesh.shape["shard"]), (*EXPERT, "shard"))
    in_specs = (P(EXPERT, None, "shard"), P("shard", EXPERT), P("shard"))
    out_specs = (P(EXPERT, None, None), P(EXPERT, None), P())
    return jax.shard_map(body, mesh=finer, in_specs=in_specs, out_specs=out_specs, check_vma=False)
```

```python
import jax
import jax.numpy as jnp
from jax import lax
from jax.experimental import pallas as pl
from jax.experimental.pallas import tpu as pltpu
from jax.sharding import Mesh
from jax.sharding import PartitionSpec as P

MESH = pl.DeviceIdType.MESH
EXPERT = ("z", "x", "core")
BF16, F32 = jnp.bfloat16, jnp.float32

BLOCK = 128
GROUPS = BLOCK // 8
PARTS = ((0, 2), (2, 7), (7, 12))
CHUNKS = ((0, 1), (1, 2), (2, 6), (6, 12))
UP_ORDER, DOWN_ORDER = (0, 1, 2, 3), (0, 1, 3, 2)
HALF = 768
SHIFT = 32
RAW = 32


def part_of(block):
    for p, (lo, hi) in enumerate(PARTS):
        if lo <= block < hi:
            return p, (block - lo) * GROUPS


def pick(first):
    lane = lax.broadcasted_iota(jnp.int32, (GROUPS, 8, 128), 2)
    group = lax.broadcasted_iota(jnp.int32, (GROUPS, 8, 128), 0)
    return lane == group + first


def column(packed, block):
    p, first = part_of(block)
    spread = jnp.where(pick(first), packed[p][None], 0.0)
    return jnp.sum(spread, axis=2, keepdims=True).reshape(BLOCK, 1)


def done(view, semaphore):
    pltpu.make_async_copy(view, view, semaphore).wait()


def gather_kernel(
    master, router, gain,
    gathered, scale_out, router_out,
    rows, raw, sums, wide, weight, gains, pieces, tall,
    load_sem, small_sem, sum_send, sum_recv, raw_send, raw_recv,
    up_send, down_send, up_recv, down_recv, group_ready, other_ready,
    row_send, row_recv, col_send, rc_recv, rx_recv, zu_recv, zd_recv,
):
    z, x, core, y = (lax.axis_index(a) for a in ("z", "x", "core", "shard"))
    nz, nx, ny = 8, 4, 4
    mine = z * (nx * 2) + x * 2 + core
    below, above = lax.rem(y + ny - 1, ny), lax.rem(y + 1, ny)
    first_raw = 12 * BLOCK - RAW

    def at_y(step):
        return (z, x, core, lax.rem(y + step, ny))

    def at_x(step):
        return (z, lax.rem(x + step, nx), core, y)

    def at_z(step):
        return (lax.rem(z + step, nz), x, core, y)

    partner = (z, x, 1 - core, y)

    def tell(semaphore, peers):
        for peer in peers:
            pl.semaphore_signal(semaphore, inc=1, device_id=peer, device_id_type=MESH)

    def send(src, dst, send_sem, recv_sem, peer):
        pltpu.make_async_remote_copy(
            src_ref=src, dst_ref=dst, send_sem=send_sem, recv_sem=recv_sem, device_id=peer, device_id_type=MESH
        ).start()

    barrier = pltpu.get_barrier_semaphore()
    gateway = y == ny - 1
    ordinary = y < ny - 1
    others = [at_z(1), at_z(nz - 1), at_x(1), at_x(nx - 1), partner]
    for d in (1, 3, 2):

        @pl.when(y + d != ny - 1)
        def _(d=d):
            tell(barrier, [at_y(d)])

    def load(at, count, k):
        view = pl.ds(at, count)
        return pltpu.make_async_copy(master.at[view], rows.at[view], load_sem.at[k])

    small = [
        pltpu.make_async_copy(router, weight, small_sem.at[0]),
        pltpu.make_async_copy(gain, gains, small_sem.at[1]),
    ]
    loads = [load(0, 256, 0), load(first_raw, RAW, 1), load(256, first_raw - 256, 2)]
    loads[0].start()
    loads[1].start()
    for copy in small:
        copy.start()
    loads[2].start()

    @pl.when(ordinary)
    def _():
        pl.semaphore_wait(barrier, ny - 1)

    @pl.when(y == ny - 2)
    def _():
        tell(group_ready, [at_y(1)])

    def partial_sums(p):
        lo, hi = PARTS[p]
        packed = jnp.zeros((8, 128), F32)
        for block in range(lo, hi):
            values = rows[pl.ds(block * BLOCK, BLOCK), :]
            total = jnp.sum(values * values, axis=1, keepdims=True).reshape(GROUPS, 8, 1)
            packed = packed + jnp.sum(jnp.where(pick((block - lo) * GROUPS), total, 0.0), axis=0)
        sums[y, p] = packed

    def send_sums(first, count, slot):
        view = sums.at[y, pl.ds(first, count)]
        for d in (2, 1, 3):
            send(view, view, sum_send, sum_recv.at[slot], at_y(d))

    loads[0].wait()
    partial_sums(0)

    @pl.when(gateway)
    def _():
        pl.semaphore_wait(group_ready, 1)

    send_sums(0, 1, 0)
    loads[1].wait()
    view = rows.at[pl.ds(first_raw, RAW)]
    send(view, raw.at[0], raw_send, raw_recv, at_y(1))
    send(view, raw.at[1], raw_send, raw_recv, at_y(ny - 1))

    @pl.when(gateway)
    def _():
        tell(barrier, others)

    loads[2].wait()
    partial_sums(1)
    partial_sums(2)
    send_sums(1, 2, 1)

    for copy in small:
        copy.wait()
    pieces[y, mine] = (weight[...] * gains[...]).astype(BF16)
    view = pieces.at[y, mine]
    for d in (1, 2, 3):
        send(view, view, row_send, row_recv, at_y(d))

    inverse = {}

    def finish_sums(slot, parts):
        done(sums.at[pl.ds(0, ny - 1), pl.ds(parts[0], len(parts))], sum_recv.at[slot])
        for p in parts:
            scale = jnp.sqrt((sums[0, p] + sums[1, p]) + (sums[2, p] + sums[3, p]))
            wide[p] = scale
            inverse[p] = 1.0 / scale

    def rescale(c):
        for block in range(*CHUNKS[c]):
            view = pl.ds(block * BLOCK, BLOCK)
            gathered[y, view, :] = (rows[view, :] * column(inverse, block)).astype(BF16)

    def send_chunk(c, upwards):
        lo, hi = CHUNKS[c][0] * BLOCK, min(CHUNKS[c][1] * BLOCK, first_raw)
        view = gathered.at[y, pl.ds(lo, hi - lo)]
        onwards = (hi <= HALF) == upwards
        k = 0 if onwards else 1
        if upwards:
            send(view, view, up_send, up_recv.at[k], at_y(1))
        else:
            send(view, view, down_send, down_recv.at[k], at_y(ny - 1))

    finish_sums(0, (0,))
    for c in (0, 1):
        rescale(c)
        send_chunk(c, True)
        send_chunk(c, False)
    finish_sums(1, (1, 2))
    rescale(2)
    send_chunk(2, True)
    rescale(3)
    send_chunk(3, False)
    send_chunk(3, True)
    send_chunk(2, False)

    done(raw, raw_recv)
    last = column(inverse, 11)[BLOCK - RAW :]
    for k, owner in enumerate((below, above)):
        gathered[owner, pl.ds(first_raw, RAW), :] = (raw[k] * last).astype(BF16)

    done(pieces.at[pl.ds(0, ny - 1), 0], row_recv)
    scales = [wide[p] for p in range(len(PARTS))]
    for block in range(12):
        same = lax.broadcasted_iota(jnp.int32, (BLOCK, 128), 0) == lax.broadcasted_iota(jnp.int32, (BLOCK, 128), 1)
        line = jnp.sum(jnp.where(same, column(scales, block), 0.0), axis=0, keepdims=True)
        scale_out[block // 6 : block // 6 + 1, (block % 6) * 128 : (block % 6 + 1) * 128] = line

    @pl.when(gateway)
    def _():
        pl.semaphore_wait(barrier, len(others))
        tell(other_ready, [at_y(d) for d in (1, 2, 3)])

    @pl.when(ordinary)
    def _():
        pl.semaphore_wait(other_ready, 1)

    view = pieces.at[:, mine]
    send(view, view, col_send, rc_recv, partner)
    done(view, rc_recv)
    view = pieces.at[:, pl.ds(z * 8 + x * 2, 2)]
    send(view, view, col_send, rx_recv.at[0], at_x(1))
    send(view, view, col_send, rx_recv.at[1], at_x(nx - 1))
    done(view, rx_recv.at[0])
    view = pieces.at[:, pl.ds(z * 8 + lax.rem(x + nx - 1, nx) * 2, 2)]
    send(view, view, col_send, rx_recv.at[1], at_x(1))
    done(pieces.at[:, pl.ds(0, 4)], rx_recv.at[1])

    def plane(step):
        return pieces.at[:, pl.ds(lax.rem(z + step, nz) * 8, 8)]

    for k in range(4):
        if k:
            done(plane(0), zu_recv.at[k - 1])
        send(plane(nz - k), plane(nz - k), col_send, zu_recv.at[k], at_z(1))
        if k < 3:
            if k:
                done(plane(0), zd_recv.at[k - 1])
            send(plane(k), plane(k), col_send, zd_recv.at[k], at_z(nz - 1))

    done(gathered.at[0, pl.ds(0, HALF)], up_recv.at[0])
    view = gathered.at[below, pl.ds(0, HALF - SHIFT)]
    send(view, view, up_send, up_recv.at[2], at_y(1))

    @pl.when(y < ny - 1)
    def _():
        view = gathered.at[below, pl.ds(HALF - SHIFT, SHIFT)]
        send(view, view, up_send, up_recv.at[2], at_y(1))

    view = gathered.at[above, pl.ds(HALF, 12 * BLOCK - HALF)]
    done(gathered.at[0, pl.ds(0, first_raw - HALF)], down_recv.at[0])
    send(view, view, down_send, down_recv.at[2], at_y(ny - 1))

    done(plane(0), zu_recv.at[3])
    done(plane(0), zd_recv.at[2])

    def lay(step, _):
        for s in range(ny):
            four = [pieces[s, step * 4 + i].astype(F32) for i in range(4)]
            tall[pl.ds(pl.multiple_of(step * 8, 8), 8), s * 512 : (s + 1) * 512] = jnp.concatenate(four, axis=0)
        return 0

    lax.fori_loop(0, 16, lay, 0)
    for i in range(16):
        router_out[i * 128 : (i + 1) * 128, :] = tall[:, i * 128 : (i + 1) * 128].T.astype(BF16)

    done(sums.at[pl.ds(0, ny - 1)], sum_send)
    done(raw, raw_send)
    done(pieces.at[pl.ds(0, ny - 1), 0], row_send)
    done(pieces.at[:, pl.ds(0, 63)], col_send)
    done(gathered.at[0, pl.ds(0, first_raw - HALF)], up_recv.at[1])
    done(gathered.at[0, pl.ds(0, HALF)], down_recv.at[1])

    @pl.when(y == 1)
    def _():
        view = gathered.at[above, pl.ds(HALF - SHIFT, SHIFT)]
        send(view, view, down_send, down_recv.at[2], at_y(ny - 1))

    def both(count):
        return gathered.at[pl.ds(0, 2), pl.ds(0, count // 2)]

    plain = first_raw + HALF
    last_ones = 12 * BLOCK - HALF

    @pl.when(y == 0)
    def _():
        done(both(plain), up_send)
        done(both(plain), down_send)
        done(gathered.at[0, pl.ds(0, last_ones + SHIFT)], down_recv.at[2])
        done(gathered.at[0, pl.ds(0, HALF - SHIFT)], up_recv.at[2])

    @pl.when(y > 0)
    def _():
        @pl.when(y == 1)
        def _():
            done(both(plain + SHIFT), down_send)

        @pl.when(y > 1)
        def _():
            done(both(plain), down_send)

        @pl.when(y == ny - 1)
        def _():
            done(both(plain - SHIFT), up_send)

        @pl.when(y < ny - 1)
        def _():
            done(both(plain), up_send)

        done(gathered.at[0, pl.ds(0, HALF)], up_recv.at[2])
        done(gathered.at[0, pl.ds(0, last_ones)], down_recv.at[2])


def write_kernel(gathered, scale, router, down_out, scale_out, router_out, sems):
    copies = [
        pltpu.make_async_copy(gathered.at[s], down_out.at[:, pl.ds(s * 512, 512)], sems.at[0]) for s in range(4)
    ]
    copies.append(pltpu.make_async_copy(scale, scale_out, sems.at[1]))
    copies.append(pltpu.make_async_copy(router, router_out, sems.at[2]))
    for copy in copies:
        copy.start()
    done(down_out, sems.at[0])
    copies[4].wait()
    copies[5].wait()


def body(master_down, router_weight, router_gain):
    dma, regular = pltpu.SemaphoreType.DMA, pltpu.SemaphoreType.REGULAR
    hbm = pl.BlockSpec(memory_space=pltpu.HBM)
    vmem = pl.BlockSpec(memory_space=pltpu.VMEM)
    gathered, scale, router = pl.pallas_call(
        gather_kernel,
        name="gather",
        out_shape=(
            pltpu.VMEM((4, 1536, 512), BF16),
            pltpu.VMEM((2, 768), F32),
            pltpu.VMEM((2048, 128), BF16),
        ),
        in_specs=[hbm] * 3,
        out_specs=[vmem] * 3,
        scratch_shapes=[
            pltpu.VMEM((1536, 512), F32),
            pltpu.VMEM((2, RAW, 512), F32),
            pltpu.VMEM((4, 3, 8, 128), F32),
            pltpu.VMEM((3, 8, 128), F32),
            pltpu.VMEM((2, 512), F32),
            pltpu.VMEM((1, 512), F32),
            pltpu.VMEM((4, 64, 2, 512), BF16),
            pltpu.VMEM((128, 2048), F32),
            dma((3,)), dma((2,)), dma(()), dma((2,)), dma(()), dma(()),
            dma(()), dma(()), dma((3,)), dma((3,)), regular, regular,
            dma(()), dma(()), dma(()), dma(()), dma((2,)), dma((4,)), dma((3,)),
        ],
        compiler_params=pltpu.CompilerParams(collective_id=0, has_side_effects=True, vmem_limit_bytes=52 << 20),
    )(master_down.reshape(1536, 512), router_weight.T, router_gain.reshape(1, 512))
    down, scale, router = pl.pallas_call(
        write_kernel,
        name="write",
        out_shape=(
            jax.ShapeDtypeStruct((1536, 2048), BF16),
            jax.ShapeDtypeStruct((2, 768), F32),
            jax.ShapeDtypeStruct((2048, 128), BF16),
        ),
        in_specs=[vmem] * 3,
        out_specs=[hbm] * 3,
        scratch_shapes=[dma((3,))],
        compiler_params=pltpu.CompilerParams(vmem_limit_bytes=1 << 20),
    )(gathered, scale, router)
    return down.reshape(2, 768, 2048), scale, router


def solution(mesh):
    finer = Mesh(mesh.devices.reshape(8, 4, 2, mesh.shape["shard"]), (*EXPERT, "shard"))
    in_specs = (P(EXPERT, None, "shard"), P("shard", EXPERT), P("shard"))
    out_specs = (P(EXPERT, None, None), P(EXPERT, None), P())
    return jax.shard_map(body, mesh=finer, in_specs=in_specs, out_specs=out_specs, check_vma=False)
```

```python
import jax
import jax.numpy as jnp
from jax import lax
from jax.experimental import pallas as pl
from jax.experimental.pallas import tpu as pltpu
from jax.sharding import Mesh
from jax.sharding import PartitionSpec as P

MESH = pl.DeviceIdType.MESH
EXPERT = ("z", "x", "core")
BF16, F32 = jnp.bfloat16, jnp.float32

BLOCK = 128
GROUPS = BLOCK // 8
PARTS = ((0, 2), (2, 7), (7, 12))
CHUNKS = ((0, 1), (1, 2), (2, 4), (4, 12))
LEAD = 512
HALF = 768
SHIFT = 32
RAW = 32


def part_of(block):
    for p, (lo, hi) in enumerate(PARTS):
        if lo <= block < hi:
            return p, (block - lo) * GROUPS


def pick(first):
    lane = lax.broadcasted_iota(jnp.int32, (GROUPS, 8, 128), 2)
    group = lax.broadcasted_iota(jnp.int32, (GROUPS, 8, 128), 0)
    return lane == group + first


def column(packed, block):
    p, first = part_of(block)
    spread = jnp.where(pick(first), packed[p][None], 0.0)
    return jnp.sum(spread, axis=2, keepdims=True).reshape(BLOCK, 1)


def done(view, semaphore):
    pltpu.make_async_copy(view, view, semaphore).wait()


def gather_kernel(
    master, router, gain,
    gathered, scale_out, router_out,
    rows, raw, sums, wide, weight, gains, pieces, tall,
    load_sem, small_sem, sum_send, sum_recv, raw_send, raw_recv,
    lead_send, rest_send, up_recv, down_recv, group_ready, other_ready, turn,
    row_send, row_recv, col_send, rc_recv, rx_recv, zu_recv, zd_recv,
):
    z, x, core, y = (lax.axis_index(a) for a in ("z", "x", "core", "shard"))
    nz, nx, ny = 8, 4, 4
    mine = z * (nx * 2) + x * 2 + core
    first_raw = 12 * BLOCK - RAW

    def at_y(step):
        return (z, x, core, lax.rem(y + step, ny))

    def at_x(step):
        return (z, lax.rem(x + step, nx), core, y)

    def at_z(step):
        return (lax.rem(z + step, nz), x, core, y)

    partner = (z, x, 1 - core, y)

    def tell(semaphore, peers):
        for peer in peers:
            pl.semaphore_signal(semaphore, inc=1, device_id=peer, device_id_type=MESH)

    def send(src, dst, send_sem, recv_sem, peer):
        pltpu.make_async_remote_copy(
            src_ref=src, dst_ref=dst, send_sem=send_sem, recv_sem=recv_sem, device_id=peer, device_id_type=MESH
        ).start()

    def both(count):
        return gathered.at[pl.ds(0, 2), pl.ds(0, count)]

    barrier = pltpu.get_barrier_semaphore()
    gateway = y == ny - 1
    ordinary = y < ny - 1
    others = [at_z(1), at_z(nz - 1), at_x(1), at_x(nx - 1), partner]
    for d in (1, 3, 2):

        @pl.when(y + d != ny - 1)
        def _(d=d):
            tell(barrier, [at_y(d)])

    def load(at, count, k):
        view = pl.ds(at, count)
        return pltpu.make_async_copy(master.at[view], rows.at[view], load_sem.at[k])

    small = [
        pltpu.make_async_copy(router, weight, small_sem.at[0]),
        pltpu.make_async_copy(gain, gains, small_sem.at[1]),
    ]
    loads = [load(0, 256, 0), load(first_raw, RAW, 1), load(256, first_raw - 256, 2)]
    loads[0].start()
    loads[1].start()
    for copy in small:
        copy.start()
    loads[2].start()

    @pl.when(ordinary)
    def _():
        pl.semaphore_wait(barrier, ny - 1)

    @pl.when(y == ny - 2)
    def _():
        tell(group_ready, [at_y(1)])

    def partial_sums(p):
        lo, hi = PARTS[p]
        packed = jnp.zeros((8, 128), F32)
        for block in range(lo, hi):
            values = rows[pl.ds(block * BLOCK, BLOCK), :]
            total = jnp.sum(values * values, axis=1, keepdims=True).reshape(GROUPS, 8, 1)
            packed = packed + jnp.sum(jnp.where(pick((block - lo) * GROUPS), total, 0.0), axis=0)
        sums[y, p] = packed

    def send_sums(first, count, slot):
        view = sums.at[y, pl.ds(first, count)]
        for d in (2, 1, 3):
            send(view, view, sum_send, sum_recv.at[slot], at_y(d))

    loads[0].wait()
    partial_sums(0)

    @pl.when(gateway)
    def _():
        pl.semaphore_wait(group_ready, 1)

    send_sums(0, 1, 0)
    loads[1].wait()
    view = rows.at[pl.ds(first_raw, RAW)]
    send(view, raw.at[0], raw_send, raw_recv, at_y(1))
    send(view, raw.at[1], raw_send, raw_recv, at_y(ny - 1))

    @pl.when(gateway)
    def _():
        tell(barrier, others)

    loads[2].wait()
    partial_sums(1)
    partial_sums(2)
    send_sums(1, 2, 1)

    for copy in small:
        copy.wait()
    pieces[y, mine] = (weight[...] * gains[...]).astype(BF16)
    view = pieces.at[y, mine]
    for d in (1, 2, 3):
        send(view, view, row_send, row_recv, at_y(d))

    inverse = {}

    def finish_sums(slot, parts):
        done(sums.at[pl.ds(0, ny - 1), pl.ds(parts[0], len(parts))], sum_recv.at[slot])
        for p in parts:
            scale = jnp.sqrt((sums[0, p] + sums[1, p]) + (sums[2, p] + sums[3, p]))
            wide[p] = scale
            inverse[p] = 1.0 / scale

    def rescale(c):
        for block in range(*CHUNKS[c]):
            view = pl.ds(block * BLOCK, BLOCK)
            gathered[0, view, :] = (rows[view, :] * column(inverse, block)).astype(BF16)

    def send_chunk(c):
        lo, hi = CHUNKS[c][0] * BLOCK, min(CHUNKS[c][1] * BLOCK, first_raw)
        here, view = gathered.at[0, pl.ds(lo, hi - lo)], pl.ds(lo, hi - lo)
        semaphore = lead_send if hi <= LEAD else rest_send
        send(here, gathered.at[1, view], semaphore, up_recv, at_y(1))
        send(here, gathered.at[2, view], semaphore, down_recv, at_y(ny - 1))

    for c in range(4):
        if c == 0:
            finish_sums(0, (0,))
        if c == 2:
            finish_sums(1, (1, 2))
        rescale(c)

        @pl.when(core == 1)
        def _(c=c):
            send_chunk(c)

    done(raw, raw_recv)
    last = column(inverse, 11)[BLOCK - RAW :]
    for k in range(2):
        gathered[k + 1, pl.ds(first_raw, RAW), :] = (raw[k] * last).astype(BF16)

    done(pieces.at[pl.ds(0, ny - 1), 0], row_recv)
    scales = [wide[p] for p in range(len(PARTS))]
    for block in range(12):
        same = lax.broadcasted_iota(jnp.int32, (BLOCK, 128), 0) == lax.broadcasted_iota(jnp.int32, (BLOCK, 128), 1)
        line = jnp.sum(jnp.where(same, column(scales, block), 0.0), axis=0, keepdims=True)
        scale_out[block // 6 : block // 6 + 1, (block % 6) * 128 : (block % 6 + 1) * 128] = line

    @pl.when(gateway)
    def _():
        pl.semaphore_wait(barrier, len(others))
        tell(other_ready, [at_y(d) for d in (1, 2, 3)])

    @pl.when(ordinary)
    def _():
        pl.semaphore_wait(other_ready, 1)

    @pl.when(core == 1)
    def _():
        done(both(LEAD), lead_send)
        tell(turn, [partner])

    @pl.when(core == 0)
    def _():
        pl.semaphore_wait(turn, 1)
        for c in range(4):
            send_chunk(c)

    view = pieces.at[:, mine]
    send(view, view, col_send, rc_recv, partner)
    done(view, rc_recv)
    view = pieces.at[:, pl.ds(z * 8 + x * 2, 2)]
    send(view, view, col_send, rx_recv.at[0], at_x(1))
    send(view, view, col_send, rx_recv.at[1], at_x(nx - 1))
    done(view, rx_recv.at[0])
    view = pieces.at[:, pl.ds(z * 8 + lax.rem(x + nx - 1, nx) * 2, 2)]
    send(view, view, col_send, rx_recv.at[1], at_x(1))
    done(pieces.at[:, pl.ds(0, 4)], rx_recv.at[1])

    def plane(step):
        return pieces.at[:, pl.ds(lax.rem(z + step, nz) * 8, 8)]

    for k in range(4):
        if k:
            done(plane(0), zu_recv.at[k - 1])
        send(plane(nz - k), plane(nz - k), col_send, zu_recv.at[k], at_z(1))
        if k < 3:
            if k:
                done(plane(0), zd_recv.at[k - 1])
            send(plane(k), plane(k), col_send, zd_recv.at[k], at_z(nz - 1))

    done(plane(0), zu_recv.at[3])
    done(plane(0), zd_recv.at[2])

    def lay(step, _):
        for s in range(ny):
            four = [pieces[s, step * 4 + i].astype(F32) for i in range(4)]
            tall[pl.ds(pl.multiple_of(step * 8, 8), 8), s * 512 : (s + 1) * 512] = jnp.concatenate(four, axis=0)
        return 0

    lax.fori_loop(0, 16, lay, 0)
    for i in range(16):
        router_out[i * 128 : (i + 1) * 128, :] = tall[:, i * 128 : (i + 1) * 128].T.astype(BF16)

    done(sums.at[pl.ds(0, ny - 1)], sum_send)
    done(raw, raw_send)
    done(pieces.at[pl.ds(0, ny - 1), 0], row_send)
    done(pieces.at[:, pl.ds(0, 63)], col_send)
    @pl.when(core == 0)
    def _():
        done(both(LEAD), lead_send)

    done(both(first_raw - LEAD), rest_send)
    done(gathered.at[0, pl.ds(0, first_raw)], up_recv)
    done(gathered.at[0, pl.ds(0, first_raw)], down_recv)


def write_kernel(gathered, scale, router, down_out, scale_out, router_out, same, sems):
    y = lax.axis_index("shard")
    copies = []
    for k, d in enumerate((0, 3, 1)):
        s = lax.rem(y + d, 4)
        columns = pl.ds(pl.multiple_of(s * 512, 512), 512)
        copies.append(pltpu.make_async_copy(gathered.at[k], down_out.at[:, columns], sems.at[0]))
    copies.append(pltpu.make_async_copy(scale, scale_out, sems.at[1]))
    copies.append(pltpu.make_async_copy(router, router_out, sems.at[2]))
    for copy in copies:
        copy.start()
    done(down_out.at[:, pl.ds(0, 3 * 512)], sems.at[0])
    copies[3].wait()
    copies[4].wait()


def forward_kernel(gathered, far, up_send, down_send, up_recv, down_recv):
    z, x, core, y = (lax.axis_index(a) for a in ("z", "x", "core", "shard"))
    ny = 4
    up, down = (z, x, core, lax.rem(y + 1, ny)), (z, x, core, lax.rem(y + ny - 1, ny))
    barrier = pltpu.get_barrier_semaphore()
    for peer in (up, down):
        pl.semaphore_signal(barrier, inc=1, device_id=peer, device_id_type=MESH)
    pl.semaphore_wait(barrier, 2)

    def send(owner, lo, hi, send_sem, recv_sem, peer):
        pltpu.make_async_remote_copy(
            src_ref=gathered.at[owner, pl.ds(lo, hi - lo)],
            dst_ref=far.at[pl.ds(lo, hi - lo)],
            send_sem=send_sem,
            recv_sem=recv_sem,
            device_id=peer,
            device_id_type=MESH,
        ).start()

    end = 12 * BLOCK
    send(1, 0, HALF - SHIFT, up_send, up_recv, up)
    send(2, HALF, end, down_send, down_recv, down)

    @pl.when(y < ny - 1)
    def _():
        send(1, HALF - SHIFT, HALF, up_send, up_recv, up)

    @pl.when(y == 1)
    def _():
        send(2, HALF - SHIFT, HALF, down_send, down_recv, down)

    @pl.when(y == ny - 1)
    def _():
        done(far.at[pl.ds(0, HALF - SHIFT)], up_send)

    @pl.when(y < ny - 1)
    def _():
        done(far.at[pl.ds(0, HALF)], up_send)

    @pl.when(y == 1)
    def _():
        done(far.at[pl.ds(0, end - HALF + SHIFT)], down_send)

    @pl.when(y != 1)
    def _():
        done(far.at[pl.ds(0, end - HALF)], down_send)

    @pl.when(y == 0)
    def _():
        done(far.at[pl.ds(0, HALF - SHIFT)], up_recv)
        done(far.at[pl.ds(0, end - HALF + SHIFT)], down_recv)

    @pl.when(y > 0)
    def _():
        done(far.at[pl.ds(0, HALF)], up_recv)
        done(far.at[pl.ds(0, end - HALF)], down_recv)


def last_kernel(down_in, far, down_out, sem):
    s = lax.rem(lax.axis_index("shard") + 2, 4)
    columns = pl.ds(pl.multiple_of(s * 512, 512), 512)
    copy = pltpu.make_async_copy(far, down_out.at[:, columns], sem)
    copy.start()
    copy.wait()


def body(master_down, router_weight, router_gain):
    dma, regular = pltpu.SemaphoreType.DMA, pltpu.SemaphoreType.REGULAR
    hbm = pl.BlockSpec(memory_space=pltpu.HBM)
    vmem = pl.BlockSpec(memory_space=pltpu.VMEM)
    gathered, scale, router = pl.pallas_call(
        gather_kernel,
        name="gather",
        out_shape=(
            pltpu.VMEM((3, 1536, 512), BF16),
            pltpu.VMEM((2, 768), F32),
            pltpu.VMEM((2048, 128), BF16),
        ),
        in_specs=[hbm] * 3,
        out_specs=[vmem] * 3,
        scratch_shapes=[
            pltpu.VMEM((1536, 512), F32),
            pltpu.VMEM((2, RAW, 512), F32),
            pltpu.VMEM((4, 3, 8, 128), F32),
            pltpu.VMEM((3, 8, 128), F32),
            pltpu.VMEM((2, 512), F32),
            pltpu.VMEM((1, 512), F32),
            pltpu.VMEM((4, 64, 2, 512), BF16),
            pltpu.VMEM((128, 2048), F32),
            dma((3,)), dma((2,)), dma(()), dma((2,)), dma(()), dma(()),
            dma(()), dma(()), dma(()), dma(()), regular, regular, regular,
            dma(()), dma(()), dma(()), dma(()), dma((2,)), dma((4,)), dma((3,)),
        ],
        compiler_params=pltpu.CompilerParams(collective_id=0, has_side_effects=True, vmem_limit_bytes=56 << 20),
    )(master_down.reshape(1536, 512), router_weight.T, router_gain.reshape(1, 512))
    down, scale, router, gathered = pl.pallas_call(
        write_kernel,
        name="write",
        out_shape=(
            jax.ShapeDtypeStruct((1536, 2048), BF16),
            jax.ShapeDtypeStruct((2, 768), F32),
            jax.ShapeDtypeStruct((2048, 128), BF16),
            pltpu.VMEM((3, 1536, 512), BF16),
        ),
        in_specs=[vmem] * 3,
        out_specs=[hbm] * 3 + [vmem],
        input_output_aliases={0: 3},
        scratch_shapes=[dma((3,))],
        compiler_params=pltpu.CompilerParams(vmem_limit_bytes=1 << 20),
    )(gathered, scale, router)
    far = pl.pallas_call(
        forward_kernel,
        name="forward",
        out_shape=pltpu.VMEM((1536, 512), BF16),
        in_specs=[vmem],
        out_specs=vmem,
        scratch_shapes=[dma(())] * 4,
        compiler_params=pltpu.CompilerParams(collective_id=1, has_side_effects=True, vmem_limit_bytes=1 << 20),
    )(gathered)
    down = pl.pallas_call(
        last_kernel,
        name="last",
        out_shape=jax.ShapeDtypeStruct((1536, 2048), BF16),
        in_specs=[hbm, vmem],
        out_specs=hbm,
        scratch_shapes=[dma(())],
        input_output_aliases={0: 0},
        compiler_params=pltpu.CompilerParams(vmem_limit_bytes=48 << 20),
    )(down, far)
    return down.reshape(2, 768, 2048), scale, router


def solution(mesh):
    finer = Mesh(mesh.devices.reshape(8, 4, 2, mesh.shape["shard"]), (*EXPERT, "shard"))
    in_specs = (P(EXPERT, None, "shard"), P("shard", EXPERT), P("shard"))
    out_specs = (P(EXPERT, None, None), P(EXPERT, None), P())
    return jax.shard_map(body, mesh=finer, in_specs=in_specs, out_specs=out_specs, check_vma=False)
```

```python
import jax
import jax.numpy as jnp
from jax import lax
from jax.experimental import pallas as pl
from jax.experimental.pallas import tpu as pltpu
from jax.sharding import Mesh
from jax.sharding import PartitionSpec as P

MESH = pl.DeviceIdType.MESH
EXPERT = ("z", "x", "core")
BF16, F32 = jnp.bfloat16, jnp.float32

BLOCK = 128
GROUPS = BLOCK // 8
PARTS = ((0, 2), (2, 7), (7, 12))
CHUNKS = ((0, 1), (1, 2), (2, 7), (7, 12))
SOON = 896
SHIFT = 32
RAW = 32


def part_of(block):
    for p, (lo, hi) in enumerate(PARTS):
        if lo <= block < hi:
            return p, (block - lo) * GROUPS


def pick(first):
    lane = lax.broadcasted_iota(jnp.int32, (GROUPS, 8, 128), 2)
    group = lax.broadcasted_iota(jnp.int32, (GROUPS, 8, 128), 0)
    return lane == group + first


def column(packed, block):
    p, first = part_of(block)
    spread = jnp.where(pick(first), packed[p][None], 0.0)
    return jnp.sum(spread, axis=2, keepdims=True).reshape(BLOCK, 1)


def done(view, semaphore):
    pltpu.make_async_copy(view, view, semaphore).wait()


def gather_kernel(
    master, router, gain,
    gathered, scale_out, router_out,
    rows, raw, sums, wide, weight, gains, pieces, tall,
    load_sem, small_sem, sum_send, sum_recv, raw_send, raw_recv,
    own_send, onward_send, up_recv, down_recv, onward_recv, group_ready, other_ready,
    row_send, row_recv, col_send, rc_recv, rx_recv, zu_recv, zd_recv,
):
    z, x, core, y = (lax.axis_index(a) for a in ("z", "x", "core", "shard"))
    nz, nx, ny = 8, 4, 4
    mine = z * (nx * 2) + x * 2 + core
    first_raw = 12 * BLOCK - RAW

    def at_y(step):
        return (z, x, core, lax.rem(y + step, ny))

    def at_x(step):
        return (z, lax.rem(x + step, nx), core, y)

    def at_z(step):
        return (lax.rem(z + step, nz), x, core, y)

    partner = (z, x, 1 - core, y)

    def tell(semaphore, peers):
        for peer in peers:
            pl.semaphore_signal(semaphore, inc=1, device_id=peer, device_id_type=MESH)

    def send(src, dst, send_sem, recv_sem, peer):
        pltpu.make_async_remote_copy(
            src_ref=src, dst_ref=dst, send_sem=send_sem, recv_sem=recv_sem, device_id=peer, device_id_type=MESH
        ).start()

    def both(count):
        return gathered.at[pl.ds(0, 2), pl.ds(0, count)]

    barrier = pltpu.get_barrier_semaphore()
    gateway = y == ny - 1
    ordinary = y < ny - 1
    others = [at_z(1), at_z(nz - 1), at_x(1), at_x(nx - 1), partner]
    for d in (1, 3, 2):

        @pl.when(y + d != ny - 1)
        def _(d=d):
            tell(barrier, [at_y(d)])

    def load(at, count, k):
        view = pl.ds(at, count)
        return pltpu.make_async_copy(master.at[view], rows.at[view], load_sem.at[k])

    small = [
        pltpu.make_async_copy(router, weight, small_sem.at[0]),
        pltpu.make_async_copy(gain, gains, small_sem.at[1]),
    ]
    loads = [load(0, 256, 0), load(first_raw, RAW, 1), load(256, first_raw - 256, 2)]
    loads[0].start()
    loads[1].start()
    for copy in small:
        copy.start()
    loads[2].start()

    @pl.when(ordinary)
    def _():
        pl.semaphore_wait(barrier, ny - 1)

    @pl.when(y == ny - 2)
    def _():
        tell(group_ready, [at_y(1)])

    def partial_sums(p):
        lo, hi = PARTS[p]
        packed = jnp.zeros((8, 128), F32)
        for block in range(lo, hi):
            values = rows[pl.ds(block * BLOCK, BLOCK), :]
            total = jnp.sum(values * values, axis=1, keepdims=True).reshape(GROUPS, 8, 1)
            packed = packed + jnp.sum(jnp.where(pick((block - lo) * GROUPS), total, 0.0), axis=0)
        sums[y, p] = packed

    def send_sums(first, count, slot):
        view = sums.at[y, pl.ds(first, count)]
        for d in (2, 1, 3):
            send(view, view, sum_send, sum_recv.at[slot], at_y(d))

    loads[0].wait()
    partial_sums(0)

    @pl.when(gateway)
    def _():
        pl.semaphore_wait(group_ready, 1)

    send_sums(0, 1, 0)
    loads[1].wait()
    view = rows.at[pl.ds(first_raw, RAW)]
    send(view, raw.at[0], raw_send, raw_recv, at_y(1))
    send(view, raw.at[1], raw_send, raw_recv, at_y(ny - 1))

    @pl.when(gateway)
    def _():
        tell(barrier, others)

    loads[2].wait()
    partial_sums(1)
    partial_sums(2)
    send_sums(1, 2, 1)

    for copy in small:
        copy.wait()
    pieces[y, mine] = (weight[...] * gains[...]).astype(BF16)
    view = pieces.at[y, mine]
    for d in (1, 2, 3):
        send(view, view, row_send, row_recv, at_y(d))

    inverse = {}

    def finish_sums(slot, parts):
        done(sums.at[pl.ds(0, ny - 1), pl.ds(parts[0], len(parts))], sum_recv.at[slot])
        for p in parts:
            scale = jnp.sqrt((sums[0, p] + sums[1, p]) + (sums[2, p] + sums[3, p]))
            wide[p] = scale
            inverse[p] = 1.0 / scale

    def rescale(c):
        for block in range(*CHUNKS[c]):
            view = pl.ds(block * BLOCK, BLOCK)
            gathered[0, view, :] = (rows[view, :] * column(inverse, block)).astype(BF16)

    def send_chunk(c):
        lo, hi = CHUNKS[c][0] * BLOCK, min(CHUNKS[c][1] * BLOCK, first_raw)
        here, view = gathered.at[0, pl.ds(lo, hi - lo)], pl.ds(lo, hi - lo)
        k = 0 if hi <= SOON else 1
        send(here, gathered.at[1, view], own_send, up_recv.at[k], at_y(1))
        send(here, gathered.at[2, view], own_send, down_recv.at[k], at_y(ny - 1))

    for c in range(4):
        if c == 0:
            finish_sums(0, (0,))
        if c == 2:
            finish_sums(1, (1, 2))
        rescale(c)

        send_chunk(c)

    done(raw, raw_recv)
    last = column(inverse, 11)[BLOCK - RAW :]
    for k in range(2):
        gathered[k + 1, pl.ds(first_raw, RAW), :] = (raw[k] * last).astype(BF16)

    done(pieces.at[pl.ds(0, ny - 1), 0], row_recv)
    scales = [wide[p] for p in range(len(PARTS))]
    for block in range(12):
        same = lax.broadcasted_iota(jnp.int32, (BLOCK, 128), 0) == lax.broadcasted_iota(jnp.int32, (BLOCK, 128), 1)
        line = jnp.sum(jnp.where(same, column(scales, block), 0.0), axis=0, keepdims=True)
        scale_out[block // 6 : block // 6 + 1, (block % 6) * 128 : (block % 6 + 1) * 128] = line

    @pl.when(gateway)
    def _():
        pl.semaphore_wait(barrier, len(others))
        tell(other_ready, [at_y(d) for d in (1, 2, 3)])

    @pl.when(ordinary)
    def _():
        pl.semaphore_wait(other_ready, 1)

    view = pieces.at[:, mine]
    send(view, view, col_send, rc_recv, partner)
    done(view, rc_recv)
    view = pieces.at[:, pl.ds(z * 8 + x * 2, 2)]
    send(view, view, col_send, rx_recv.at[0], at_x(1))
    send(view, view, col_send, rx_recv.at[1], at_x(nx - 1))
    done(view, rx_recv.at[0])
    view = pieces.at[:, pl.ds(z * 8 + lax.rem(x + nx - 1, nx) * 2, 2)]
    send(view, view, col_send, rx_recv.at[1], at_x(1))
    done(pieces.at[:, pl.ds(0, 4)], rx_recv.at[1])

    def plane(step):
        return pieces.at[:, pl.ds(lax.rem(z + step, nz) * 8, 8)]

    for k in range(4):
        if k:
            done(plane(0), zu_recv.at[k - 1])
        send(plane(nz - k), plane(nz - k), col_send, zu_recv.at[k], at_z(1))
        if k < 3:
            if k:
                done(plane(0), zd_recv.at[k - 1])
            send(plane(k), plane(k), col_send, zd_recv.at[k], at_z(nz - 1))

    done(gathered.at[0, pl.ds(0, SOON)], up_recv.at[0])
    done(gathered.at[0, pl.ds(0, SOON)], down_recv.at[0])

    @pl.when(core == 0)
    def _():
        lower, upper = pl.ds(0, SOON // 2), pl.ds(SOON // 2, SOON // 2)
        send(gathered.at[1, lower], gathered.at[3, lower], onward_send, onward_recv, at_y(1))
        send(gathered.at[2, upper], gathered.at[3, upper], onward_send, onward_recv, at_y(ny - 1))

    done(plane(0), zu_recv.at[3])
    done(plane(0), zd_recv.at[2])

    def lay(step, _):
        for s in range(ny):
            four = [pieces[s, step * 4 + i].astype(F32) for i in range(4)]
            tall[pl.ds(pl.multiple_of(step * 8, 8), 8), s * 512 : (s + 1) * 512] = jnp.concatenate(four, axis=0)
        return 0

    lax.fori_loop(0, 16, lay, 0)
    for i in range(16):
        router_out[i * 128 : (i + 1) * 128, :] = tall[:, i * 128 : (i + 1) * 128].T.astype(BF16)

    done(sums.at[pl.ds(0, ny - 1)], sum_send)
    done(raw, raw_send)
    done(pieces.at[pl.ds(0, ny - 1), 0], row_send)
    done(pieces.at[:, pl.ds(0, 63)], col_send)
    done(both(first_raw), own_send)
    done(gathered.at[0, pl.ds(0, first_raw - SOON)], up_recv.at[1])
    done(gathered.at[0, pl.ds(0, first_raw - SOON)], down_recv.at[1])

    @pl.when(core == 0)
    def _():
        done(gathered.at[0, pl.ds(0, SOON)], onward_send)
        done(gathered.at[0, pl.ds(0, SOON)], onward_recv)


def write_kernel(gathered, scale, router, down_out, scale_out, router_out, same, sems):
    y = lax.axis_index("shard")
    copies = []
    for k, d in enumerate((0, 3, 1)):
        s = lax.rem(y + d, 4)
        columns = pl.ds(pl.multiple_of(s * 512, 512), 512)
        copies.append(pltpu.make_async_copy(gathered.at[k], down_out.at[:, columns], sems.at[0]))
    copies.append(pltpu.make_async_copy(scale, scale_out, sems.at[1]))
    copies.append(pltpu.make_async_copy(router, router_out, sems.at[2]))
    for copy in copies:
        copy.start()

    @pl.when(lax.axis_index("core") == 0)
    def _():
        columns = pl.ds(pl.multiple_of(lax.rem(y + 2, 4) * 512, 512), 512)
        view = pl.ds(0, SOON)
        copy = pltpu.make_async_copy(gathered.at[3, view], down_out.at[view, columns], sems.at[3])
        copy.start()
        copy.wait()

    done(down_out.at[:, pl.ds(0, 3 * 512)], sems.at[0])
    copies[3].wait()
    copies[4].wait()


def forward_kernel(gathered, far, up_send, down_send, up_recv, down_recv):
    z, x, core, y = (lax.axis_index(a) for a in ("z", "x", "core", "shard"))
    ny = 4
    up, down = (z, x, core, lax.rem(y + 1, ny)), (z, x, core, lax.rem(y + ny - 1, ny))
    barrier = pltpu.get_barrier_semaphore()
    for peer in (up, down):
        pl.semaphore_signal(barrier, inc=1, device_id=peer, device_id_type=MESH)
    pl.semaphore_wait(barrier, 2)

    def send(owner, lo, hi, send_sem, recv_sem, peer):
        pltpu.make_async_remote_copy(
            src_ref=gathered.at[owner, pl.ds(lo, hi - lo)],
            dst_ref=far.at[pl.ds(lo, hi - lo)],
            send_sem=send_sem,
            recv_sem=recv_sem,
            device_id=peer,
            device_id_type=MESH,
        ).start()

    def onwards(first):
        end = 12 * BLOCK
        half = (first + end) // 2
        send(1, first, half - SHIFT, up_send, up_recv, up)
        send(2, half, end, down_send, down_recv, down)

        @pl.when(y < ny - 1)
        def _():
            send(1, half - SHIFT, half, up_send, up_recv, up)

        @pl.when(y == 1)
        def _():
            send(2, half - SHIFT, half, down_send, down_recv, down)

        @pl.when(y == ny - 1)
        def _():
            done(far.at[pl.ds(0, half - SHIFT - first)], up_send)

        @pl.when(y < ny - 1)
        def _():
            done(far.at[pl.ds(0, half - first)], up_send)

        @pl.when(y == 1)
        def _():
            done(far.at[pl.ds(0, end - half + SHIFT)], down_send)

        @pl.when(y != 1)
        def _():
            done(far.at[pl.ds(0, end - half)], down_send)

        @pl.when(y == 0)
        def _():
            done(far.at[pl.ds(0, half - SHIFT - first)], up_recv)
            done(far.at[pl.ds(0, end - half + SHIFT)], down_recv)

        @pl.when(y > 0)
        def _():
            done(far.at[pl.ds(0, half - first)], up_recv)
            done(far.at[pl.ds(0, end - half)], down_recv)

    @pl.when(core == 0)
    def _():
        onwards(SOON)

    @pl.when(core == 1)
    def _():
        onwards(0)


def last_kernel(down_in, far, down_out, sem):
    s = lax.rem(lax.axis_index("shard") + 2, 4)
    columns = pl.ds(pl.multiple_of(s * 512, 512), 512)
    for core, first in ((0, SOON), (1, 0)):

        @pl.when(lax.axis_index("core") == core)
        def _(first=first):
            view = pl.ds(first, 12 * BLOCK - first)
            copy = pltpu.make_async_copy(far.at[view], down_out.at[view, columns], sem)
            copy.start()
            copy.wait()


def body(master_down, router_weight, router_gain):
    dma, regular = pltpu.SemaphoreType.DMA, pltpu.SemaphoreType.REGULAR
    hbm = pl.BlockSpec(memory_space=pltpu.HBM)
    vmem = pl.BlockSpec(memory_space=pltpu.VMEM)
    gathered, scale, router = pl.pallas_call(
        gather_kernel,
        name="gather",
        out_shape=(
            pltpu.VMEM((4, 1536, 512), BF16),
            pltpu.VMEM((2, 768), F32),
            pltpu.VMEM((2048, 128), BF16),
        ),
        in_specs=[hbm] * 3,
        out_specs=[vmem] * 3,
        scratch_shapes=[
            pltpu.VMEM((1536, 512), F32),
            pltpu.VMEM((2, RAW, 512), F32),
            pltpu.VMEM((4, 3, 8, 128), F32),
            pltpu.VMEM((3, 8, 128), F32),
            pltpu.VMEM((2, 512), F32),
            pltpu.VMEM((1, 512), F32),
            pltpu.VMEM((4, 64, 2, 512), BF16),
            pltpu.VMEM((128, 2048), F32),
            dma((3,)), dma((2,)), dma(()), dma((2,)), dma(()), dma(()),
            dma(()), dma(()), dma((2,)), dma((2,)), dma(()), regular, regular,
            dma(()), dma(()), dma(()), dma(()), dma((2,)), dma((4,)), dma((3,)),
        ],
        compiler_params=pltpu.CompilerParams(collective_id=0, has_side_effects=True, vmem_limit_bytes=56 << 20),
    )(master_down.reshape(1536, 512), router_weight.T, router_gain.reshape(1, 512))
    down, scale, router, gathered = pl.pallas_call(
        write_kernel,
        name="write",
        out_shape=(
            jax.ShapeDtypeStruct((1536, 2048), BF16),
            jax.ShapeDtypeStruct((2, 768), F32),
            jax.ShapeDtypeStruct((2048, 128), BF16),
            pltpu.VMEM((4, 1536, 512), BF16),
        ),
        in_specs=[vmem] * 3,
        out_specs=[hbm] * 3 + [vmem],
        input_output_aliases={0: 3},
        scratch_shapes=[dma((4,))],
        compiler_params=pltpu.CompilerParams(vmem_limit_bytes=1 << 20),
    )(gathered, scale, router)
    far = pl.pallas_call(
        forward_kernel,
        name="forward",
        out_shape=pltpu.VMEM((1536, 512), BF16),
        in_specs=[vmem],
        out_specs=vmem,
        scratch_shapes=[dma(())] * 4,
        compiler_params=pltpu.CompilerParams(collective_id=1, has_side_effects=True, vmem_limit_bytes=1 << 20),
    )(gathered)
    down = pl.pallas_call(
        last_kernel,
        name="last",
        out_shape=jax.ShapeDtypeStruct((1536, 2048), BF16),
        in_specs=[hbm, vmem],
        out_specs=hbm,
        scratch_shapes=[dma(())],
        input_output_aliases={0: 0},
        compiler_params=pltpu.CompilerParams(vmem_limit_bytes=48 << 20),
    )(down, far)
    return down.reshape(2, 768, 2048), scale, router


def solution(mesh):
    finer = Mesh(mesh.devices.reshape(8, 4, 2, mesh.shape["shard"]), (*EXPERT, "shard"))
    in_specs = (P(EXPERT, None, "shard"), P("shard", EXPERT), P("shard"))
    out_specs = (P(EXPERT, None, None), P(EXPERT, None), P())
    return jax.shard_map(body, mesh=finer, in_specs=in_specs, out_specs=out_specs, check_vma=False)
```

```python
import jax
import jax.numpy as jnp
from jax import lax
from jax.experimental import pallas as pl
from jax.experimental.pallas import tpu as pltpu
from jax.sharding import Mesh
from jax.sharding import PartitionSpec as P

MESH = pl.DeviceIdType.MESH
EXPERT = ("z", "x", "core")
BF16, F32 = jnp.bfloat16, jnp.float32

BLOCK = 128
GROUPS = BLOCK // 8
PARTS = ((0, 2), (2, 7), (7, 12))
CHUNKS = ((0, 1), (1, 2), (2, 7), (7, 12))
SOON = 896
SHIFT = 32
RAW = 48


def part_of(block):
    for p, (lo, hi) in enumerate(PARTS):
        if lo <= block < hi:
            return p, (block - lo) * GROUPS


def pick(first):
    lane = lax.broadcasted_iota(jnp.int32, (GROUPS, 8, 128), 2)
    group = lax.broadcasted_iota(jnp.int32, (GROUPS, 8, 128), 0)
    return lane == group + first


def column(packed, block):
    p, first = part_of(block)
    spread = jnp.where(pick(first), packed[p][None], 0.0)
    return jnp.sum(spread, axis=2, keepdims=True).reshape(BLOCK, 1)


def done(view, semaphore):
    pltpu.make_async_copy(view, view, semaphore).wait()


def gather_kernel(
    master, router, gain,
    gathered, scale_out, router_out,
    rows, raw, sums, wide, weight, gains, pieces, tall,
    load_sem, small_sem, sum_send, sum_recv, raw_send, raw_recv,
    own_send, onward_send, up_recv, down_recv, onward_recv, group_ready, other_ready,
    row_send, row_recv, col_send, rc_recv, rx_recv, zu_recv, zd_recv,
):
    z, x, core, y = (lax.axis_index(a) for a in ("z", "x", "core", "shard"))
    nz, nx, ny = 8, 4, 4
    mine = z * (nx * 2) + x * 2 + core
    first_raw = 12 * BLOCK - RAW

    def at_y(step):
        return (z, x, core, lax.rem(y + step, ny))

    def at_x(step):
        return (z, lax.rem(x + step, nx), core, y)

    def at_z(step):
        return (lax.rem(z + step, nz), x, core, y)

    partner = (z, x, 1 - core, y)

    def tell(semaphore, peers):
        for peer in peers:
            pl.semaphore_signal(semaphore, inc=1, device_id=peer, device_id_type=MESH)

    def send(src, dst, send_sem, recv_sem, peer):
        pltpu.make_async_remote_copy(
            src_ref=src, dst_ref=dst, send_sem=send_sem, recv_sem=recv_sem, device_id=peer, device_id_type=MESH
        ).start()

    def both(count):
        return gathered.at[pl.ds(0, 2), pl.ds(0, count)]

    barrier = pltpu.get_barrier_semaphore()
    gateway = y == ny - 1
    ordinary = y < ny - 1
    others = [at_z(1), at_z(nz - 1), at_x(1), at_x(nx - 1), partner]
    for d in (1, 3, 2):

        @pl.when(y + d != ny - 1)
        def _(d=d):
            tell(barrier, [at_y(d)])

    def load(at, count, k):
        view = pl.ds(at, count)
        return pltpu.make_async_copy(master.at[view], rows.at[view], load_sem.at[k])

    small = [
        pltpu.make_async_copy(router, weight, small_sem.at[0]),
        pltpu.make_async_copy(gain, gains, small_sem.at[1]),
    ]
    loads = [load(0, 256, 0), load(first_raw, RAW, 1), load(256, first_raw - 256, 2)]
    loads[0].start()
    loads[1].start()
    for copy in small:
        copy.start()
    loads[2].start()

    @pl.when(ordinary)
    def _():
        pl.semaphore_wait(barrier, ny - 1)

    @pl.when(y == ny - 2)
    def _():
        tell(group_ready, [at_y(1)])

    def partial_sums(p):
        lo, hi = PARTS[p]
        packed = jnp.zeros((8, 128), F32)
        for block in range(lo, hi):
            values = rows[pl.ds(block * BLOCK, BLOCK), :]
            total = jnp.sum(values * values, axis=1, keepdims=True).reshape(GROUPS, 8, 1)
            packed = packed + jnp.sum(jnp.where(pick((block - lo) * GROUPS), total, 0.0), axis=0)
        sums[y, p] = packed

    def send_sums(first, count, slot):
        view = sums.at[y, pl.ds(first, count)]
        for d in (2, 1, 3):
            send(view, view, sum_send, sum_recv.at[slot], at_y(d))

    loads[0].wait()
    partial_sums(0)

    @pl.when(gateway)
    def _():
        pl.semaphore_wait(group_ready, 1)

    send_sums(0, 1, 0)
    loads[1].wait()
    view = rows.at[pl.ds(first_raw, RAW)]
    send(view, raw.at[0], raw_send, raw_recv, at_y(1))
    send(view, raw.at[1], raw_send, raw_recv, at_y(ny - 1))

    @pl.when(gateway)
    def _():
        tell(barrier, others)

    loads[2].wait()
    partial_sums(1)
    partial_sums(2)
    send_sums(1, 2, 1)

    for copy in small:
        copy.wait()
    pieces[y, mine] = (weight[...] * gains[...]).astype(BF16)
    view = pieces.at[y, mine]
    for d in (1, 2, 3):
        send(view, view, row_send, row_recv, at_y(d))

    inverse = {}

    def finish_sums(slot, parts):
        done(sums.at[pl.ds(0, ny - 1), pl.ds(parts[0], len(parts))], sum_recv.at[slot])
        for p in parts:
            scale = jnp.sqrt((sums[0, p] + sums[1, p]) + (sums[2, p] + sums[3, p]))
            wide[p] = scale
            inverse[p] = 1.0 / scale

    def rescale(c):
        for block in range(*CHUNKS[c]):
            view = pl.ds(block * BLOCK, BLOCK)
            gathered[0, view, :] = (rows[view, :] * column(inverse, block)).astype(BF16)

    def send_chunk(c):
        lo, hi = CHUNKS[c][0] * BLOCK, min(CHUNKS[c][1] * BLOCK, first_raw)
        here, view = gathered.at[0, pl.ds(lo, hi - lo)], pl.ds(lo, hi - lo)
        k = 0 if hi <= SOON else 1
        send(here, gathered.at[1, view], own_send, up_recv.at[k], at_y(1))
        send(here, gathered.at[2, view], own_send, down_recv.at[k], at_y(ny - 1))

    for c in range(4):
        if c == 0:
            finish_sums(0, (0,))
        if c == 2:
            finish_sums(1, (1, 2))
        rescale(c)

        send_chunk(c)

    done(raw, raw_recv)
    last = column(inverse, 11)[BLOCK - RAW :]
    for k in range(2):
        gathered[k + 1, pl.ds(first_raw, RAW), :] = (raw[k] * last).astype(BF16)

    done(pieces.at[pl.ds(0, ny - 1), 0], row_recv)
    scales = [wide[p] for p in range(len(PARTS))]
    for block in range(12):
        same = lax.broadcasted_iota(jnp.int32, (BLOCK, 128), 0) == lax.broadcasted_iota(jnp.int32, (BLOCK, 128), 1)
        line = jnp.sum(jnp.where(same, column(scales, block), 0.0), axis=0, keepdims=True)
        scale_out[block // 6 : block // 6 + 1, (block % 6) * 128 : (block % 6 + 1) * 128] = line

    @pl.when(gateway)
    def _():
        pl.semaphore_wait(barrier, len(others))
        tell(other_ready, [at_y(d) for d in (1, 2, 3)])

    @pl.when(ordinary)
    def _():
        pl.semaphore_wait(other_ready, 1)

    view = pieces.at[:, mine]
    send(view, view, col_send, rc_recv, partner)
    done(view, rc_recv)
    view = pieces.at[:, pl.ds(z * 8 + x * 2, 2)]
    send(view, view, col_send, rx_recv.at[0], at_x(1))
    send(view, view, col_send, rx_recv.at[1], at_x(nx - 1))
    done(view, rx_recv.at[0])
    view = pieces.at[:, pl.ds(z * 8 + lax.rem(x + nx - 1, nx) * 2, 2)]
    send(view, view, col_send, rx_recv.at[1], at_x(1))
    done(pieces.at[:, pl.ds(0, 4)], rx_recv.at[1])

    def plane(step):
        return pieces.at[:, pl.ds(lax.rem(z + step, nz) * 8, 8)]

    for k in range(4):
        if k:
            done(plane(0), zu_recv.at[k - 1])
        send(plane(nz - k), plane(nz - k), col_send, zu_recv.at[k], at_z(1))
        if k < 3:
            if k:
                done(plane(0), zd_recv.at[k - 1])
            send(plane(k), plane(k), col_send, zd_recv.at[k], at_z(nz - 1))

    done(gathered.at[0, pl.ds(0, SOON)], up_recv.at[0])
    done(gathered.at[0, pl.ds(0, SOON)], down_recv.at[0])

    @pl.when(core == 0)
    def _():
        lower, upper = pl.ds(0, SOON // 2), pl.ds(SOON // 2, SOON // 2)
        send(gathered.at[1, lower], gathered.at[3, lower], onward_send, onward_recv, at_y(1))
        send(gathered.at[2, upper], gathered.at[3, upper], onward_send, onward_recv, at_y(ny - 1))

    done(plane(0), zu_recv.at[3])
    done(plane(0), zd_recv.at[2])

    def lay(step, _):
        for s in range(ny):
            four = [pieces[s, step * 4 + i].astype(F32) for i in range(4)]
            tall[pl.ds(pl.multiple_of(step * 8, 8), 8), s * 512 : (s + 1) * 512] = jnp.concatenate(four, axis=0)
        return 0

    lax.fori_loop(0, 16, lay, 0)
    for i in range(16):
        router_out[i * 128 : (i + 1) * 128, :] = tall[:, i * 128 : (i + 1) * 128].T.astype(BF16)

    done(sums.at[pl.ds(0, ny - 1)], sum_send)
    done(raw, raw_send)
    done(pieces.at[pl.ds(0, ny - 1), 0], row_send)
    done(pieces.at[:, pl.ds(0, 63)], col_send)
    done(both(first_raw), own_send)
    done(gathered.at[0, pl.ds(0, first_raw - SOON)], up_recv.at[1])
    done(gathered.at[0, pl.ds(0, first_raw - SOON)], down_recv.at[1])

    @pl.when(core == 0)
    def _():
        done(gathered.at[0, pl.ds(0, SOON)], onward_send)
        done(gathered.at[0, pl.ds(0, SOON)], onward_recv)


def write_kernel(gathered, scale, router, down_out, scale_out, router_out, same, sems):
    y = lax.axis_index("shard")
    copies = []
    for k, d in enumerate((0, 3, 1)):
        s = lax.rem(y + d, 4)
        columns = pl.ds(pl.multiple_of(s * 512, 512), 512)
        copies.append(pltpu.make_async_copy(gathered.at[k], down_out.at[:, columns], sems.at[0]))
    copies.append(pltpu.make_async_copy(scale, scale_out, sems.at[1]))
    copies.append(pltpu.make_async_copy(router, router_out, sems.at[2]))
    for copy in copies:
        copy.start()

    @pl.when(lax.axis_index("core") == 0)
    def _():
        columns = pl.ds(pl.multiple_of(lax.rem(y + 2, 4) * 512, 512), 512)
        view = pl.ds(0, SOON)
        copy = pltpu.make_async_copy(gathered.at[3, view], down_out.at[view, columns], sems.at[3])
        copy.start()
        copy.wait()

    done(down_out.at[:, pl.ds(0, 3 * 512)], sems.at[0])
    copies[3].wait()
    copies[4].wait()


def forward_kernel(gathered, far, up_send, down_send, up_recv, down_recv):
    z, x, core, y = (lax.axis_index(a) for a in ("z", "x", "core", "shard"))
    ny = 4
    up, down = (z, x, core, lax.rem(y + 1, ny)), (z, x, core, lax.rem(y + ny - 1, ny))
    barrier = pltpu.get_barrier_semaphore()
    for peer in (up, down):
        pl.semaphore_signal(barrier, inc=1, device_id=peer, device_id_type=MESH)
    pl.semaphore_wait(barrier, 2)

    def send(owner, lo, hi, send_sem, recv_sem, peer):
        pltpu.make_async_remote_copy(
            src_ref=gathered.at[owner, pl.ds(lo, hi - lo)],
            dst_ref=far.at[pl.ds(lo, hi - lo)],
            send_sem=send_sem,
            recv_sem=recv_sem,
            device_id=peer,
            device_id_type=MESH,
        ).start()

    def onwards(first):
        end = 12 * BLOCK
        half = (first + end) // 2
        send(1, first, half - SHIFT, up_send, up_recv, up)
        send(2, half, end, down_send, down_recv, down)

        @pl.when(y < ny - 1)
        def _():
            send(1, half - SHIFT, half, up_send, up_recv, up)

        @pl.when(y == 1)
        def _():
            send(2, half - SHIFT, half, down_send, down_recv, down)

        @pl.when(y == ny - 1)
        def _():
            done(far.at[pl.ds(0, half - SHIFT - first)], up_send)

        @pl.when(y < ny - 1)
        def _():
            done(far.at[pl.ds(0, half - first)], up_send)

        @pl.when(y == 1)
        def _():
            done(far.at[pl.ds(0, end - half + SHIFT)], down_send)

        @pl.when(y != 1)
        def _():
            done(far.at[pl.ds(0, end - half)], down_send)

        @pl.when(y == 0)
        def _():
            done(far.at[pl.ds(0, half - SHIFT - first)], up_recv)
            done(far.at[pl.ds(0, end - half + SHIFT)], down_recv)

        @pl.when(y > 0)
        def _():
            done(far.at[pl.ds(0, half - first)], up_recv)
            done(far.at[pl.ds(0, end - half)], down_recv)

    @pl.when(core == 0)
    def _():
        onwards(SOON)

    @pl.when(core == 1)
    def _():
        onwards(0)


def last_kernel(down_in, far, down_out, sem):
    s = lax.rem(lax.axis_index("shard") + 2, 4)
    columns = pl.ds(pl.multiple_of(s * 512, 512), 512)
    for core, first in ((0, SOON), (1, 0)):

        @pl.when(lax.axis_index("core") == core)
        def _(first=first):
            view = pl.ds(first, 12 * BLOCK - first)
            copy = pltpu.make_async_copy(far.at[view], down_out.at[view, columns], sem)
            copy.start()
            copy.wait()


def body(master_down, router_weight, router_gain):
    dma, regular = pltpu.SemaphoreType.DMA, pltpu.SemaphoreType.REGULAR
    hbm = pl.BlockSpec(memory_space=pltpu.HBM)
    vmem = pl.BlockSpec(memory_space=pltpu.VMEM)
    gathered, scale, router = pl.pallas_call(
        gather_kernel,
        name="gather",
        out_shape=(
            pltpu.VMEM((4, 1536, 512), BF16),
            pltpu.VMEM((2, 768), F32),
            pltpu.VMEM((2048, 128), BF16),
        ),
        in_specs=[hbm] * 3,
        out_specs=[vmem] * 3,
        scratch_shapes=[
            pltpu.VMEM((1536, 512), F32),
            pltpu.VMEM((2, RAW, 512), F32),
            pltpu.VMEM((4, 3, 8, 128), F32),
            pltpu.VMEM((3, 8, 128), F32),
            pltpu.VMEM((2, 512), F32),
            pltpu.VMEM((1, 512), F32),
            pltpu.VMEM((4, 64, 2, 512), BF16),
            pltpu.VMEM((128, 2048), F32),
            dma((3,)), dma((2,)), dma(()), dma((2,)), dma(()), dma(()),
            dma(()), dma(()), dma((2,)), dma((2,)), dma(()), regular, regular,
            dma(()), dma(()), dma(()), dma(()), dma((2,)), dma((4,)), dma((3,)),
        ],
        compiler_params=pltpu.CompilerParams(collective_id=0, has_side_effects=True, vmem_limit_bytes=56 << 20),
    )(master_down.reshape(1536, 512), router_weight.T, router_gain.reshape(1, 512))
    down, scale, router, gathered = pl.pallas_call(
        write_kernel,
        name="write",
        out_shape=(
            jax.ShapeDtypeStruct((1536, 2048), BF16),
            jax.ShapeDtypeStruct((2, 768), F32),
            jax.ShapeDtypeStruct((2048, 128), BF16),
            pltpu.VMEM((4, 1536, 512), BF16),
        ),
        in_specs=[vmem] * 3,
        out_specs=[hbm] * 3 + [vmem],
        input_output_aliases={0: 3},
        scratch_shapes=[dma((4,))],
        compiler_params=pltpu.CompilerParams(vmem_limit_bytes=1 << 20),
    )(gathered, scale, router)
    far = pl.pallas_call(
        forward_kernel,
        name="forward",
        out_shape=pltpu.VMEM((1536, 512), BF16),
        in_specs=[vmem],
        out_specs=vmem,
        scratch_shapes=[dma(())] * 4,
        compiler_params=pltpu.CompilerParams(collective_id=1, has_side_effects=True, vmem_limit_bytes=1 << 20),
    )(gathered)
    down = pl.pallas_call(
        last_kernel,
        name="last",
        out_shape=jax.ShapeDtypeStruct((1536, 2048), BF16),
        in_specs=[hbm, vmem],
        out_specs=hbm,
        scratch_shapes=[dma(())],
        input_output_aliases={0: 0},
        compiler_params=pltpu.CompilerParams(vmem_limit_bytes=48 << 20),
    )(down, far)
    return down.reshape(2, 768, 2048), scale, router


def solution(mesh):
    finer = Mesh(mesh.devices.reshape(8, 4, 2, mesh.shape["shard"]), (*EXPERT, "shard"))
    in_specs = (P(EXPERT, None, "shard"), P("shard", EXPERT), P("shard"))
    out_specs = (P(EXPERT, None, None), P(EXPERT, None), P())
    return jax.shard_map(body, mesh=finer, in_specs=in_specs, out_specs=out_specs, check_vma=False)
```
